32 devices in a mesh: col: 16 (over z, y, x), sec: 2 (over core).
Axes of the slice: x: 2, y: 2, z: 4, core: 2. Of those that a mesh axis runs over, the one named last changes fastest.
Arguments:
- mps: bfloat16 [16, 96, 6, 6, 96], P('col', 'sec'), may hold values from -6 to 6
- ket: bfloat16 [16, 6, 6, 6, 6, 2], P('col'), may hold values from -6 to 6
- left_proj: bfloat16 [16, 96, 96, 6, 6], P('col', 'sec'), may hold values from -0.109375 to 0.109375
- right_proj: bfloat16 [16, 96, 6, 6, 96], P('col', None, None, None, 'sec'), may hold values from -0.109375 to 0.109375
- bond_charge: int32 [16, 96], P('col'), may hold values from 0 to 5
- new_charge: int32 [16, 96], P('col'), may hold values from 0 to 5
- link_charge: int32 [16, 6], P('col'), may hold values from 0 to 2
- vert_charge: int32 [16, 2, 6], P('col'), may hold values from 0 to 2
Outputs:
- new_mps: bfloat16 [16, 96, 6, 6, 96], P('col', 'sec')
- log_norm: float32 [], replicated
The draws below stay inside these ranges and needn't reach their ends.
All inputs are finite; a program needn't handle non-finite values.
Results may differ from the reference program's by a relative error of at most 0.0064.
Values may be sent and summed in bfloat16 or wider, within the bound.
No kernel may reach another device: no remote copies, remote signals or barrier semaphores. Data moves between devices by JAX's collectives and lax.ppermute only.
A program may use at most 192 MiB of HBM per device.

```python
import jax
import jax.numpy as jnp
from jax import lax

CHI = 96
D = 6
P_SIZE = 2
SITES = 16


def with_ends(values, key, least, top_value):
    dims = values.shape
    index_at = [jax.random.randint(jax.random.fold_in(key, axis), (), 0, dims[axis]) for axis in range(len(dims))]
    values = values.at[tuple(index_at)].set(least)
    longest = dims.index(max(dims))
    index_at[longest] = (index_at[longest] + 1) % dims[longest]
    return values.at[tuple(index_at)].set(top_value)


def steps_of(rng, extent, split, low, largest):
    loudness = 1.0
    for dim, blocks in split:
        draws = jax.random.uniform(jax.random.fold_in(jax.random.fold_in(rng, 6), dim), (blocks,), jnp.float32, low / len(split), largest / len(split))
        loudness = loudness * jnp.repeat(jnp.exp(draws), extent[dim] // blocks).reshape((-1,) + (1,) * (len(extent) - 1 - dim))
    return loudness


def normal_values(stream_key, extent, deviation, most, cuts=(), held_as=jnp.bfloat16):
    entries = jax.random.normal(stream_key, extent, jnp.float32) * deviation
    if len(cuts) > 0:
        entries = steps_of(stream_key, extent, cuts, -0.22, 0.18) * entries
    return jnp.clip(entries, min=-most, max=most).astype(held_as)


def setup_inputs(seed: int = 0) -> dict:
    key_of = jax.random.split(jax.random.key(seed), 9)
    return {
        "mps": normal_values(key_of[0], (SITES, CHI, D, D, CHI), 1.0, 6.0, ((0, 16), (1, 2))),
        "ket": normal_values(key_of[1], (SITES, D, D, D, D, P_SIZE), 1.0, 6.0, ((0, 16),)),
        "left_proj": normal_values(key_of[2], (SITES, CHI, CHI, D, D), (CHI * D * D) ** -0.5, 0.109375, ((0, 16), (1, 2))),
        "right_proj": normal_values(key_of[3], (SITES, CHI, D, D, CHI), (CHI * D * D) ** -0.5, 0.109375, ((0, 16), (4, 2))),
        "bond_charge": with_ends(jax.random.randint(key_of[4], (SITES, CHI), 0, 6), jax.random.fold_in(key_of[4], 1), 0, 5).astype(jnp.int32),
        "new_charge": with_ends(jax.random.randint(key_of[5], (SITES, CHI), 0, 6), jax.random.fold_in(key_of[5], 1), 0, 5).astype(jnp.int32),
        "link_charge": with_ends(jax.random.randint(key_of[6], (SITES, D), 0, 3), jax.random.fold_in(key_of[6], 1), 0, 2).astype(jnp.int32),
        "vert_charge": with_ends(jax.random.randint(key_of[7], (SITES, 2, D), 0, 3), jax.random.fold_in(key_of[7], 1), 0, 2).astype(jnp.int32),
    }


def absorb(mps_site, ket_site, left_site, right_site, charge_here, charge_next, fresh_here, fresh_next, link_here, link_next, vertical):
    upper = vertical[0]
    lower = vertical[1]
    physical = jnp.arange(ket_site.shape[4], dtype=jnp.int32)
    keep_mps = charge_here[:, None, None, None] + upper[None, :, None, None] - upper[None, None, :, None] == charge_next[None, None, None, :]
    masked_mps = jnp.where(keep_mps, mps_site, jnp.zeros_like(mps_site))
    keep_ket = upper[:, None, None, None, None] + link_here[None, :, None, None, None] == lower[None, None, :, None, None] + link_next[None, None, None, :, None] + physical[None, None, None, None, :]
    masked_ket = jnp.where(keep_ket, ket_site, jnp.zeros_like(ket_site))
    keep_left = fresh_here[:, None, None, None] == charge_here[None, :, None, None] + link_here[None, None, :, None] - link_here[None, None, None, :]
    masked_left = jnp.where(keep_left, left_site, jnp.zeros_like(left_site))
    keep_right = charge_next[:, None, None, None] + link_next[None, :, None, None] - link_next[None, None, :, None] == fresh_next[None, None, None, :]
    masked_right = jnp.where(keep_right, right_site, jnp.zeros_like(right_site))
    ket_wide = masked_ket.astype(jnp.float32)
    first = jnp.einsum('xalm,auvb->xlmuvb', masked_left.astype(jnp.float32), masked_mps.astype(jnp.float32)).astype(jnp.bfloat16)
    second = jnp.einsum('xlmuvb,uldrp->xmvbdrp', first.astype(jnp.float32), ket_wide).astype(jnp.bfloat16)
    third = jnp.einsum('xmvbdrp,vmesp->xbdres', second.astype(jnp.float32), ket_wide).astype(jnp.bfloat16)
    return jnp.einsum('xbdres,brsy->xdey', third.astype(jnp.float32), masked_right.astype(jnp.float32))

def reference(mps, ket, left_proj, right_proj, bond_charge, new_charge, link_charge, vert_charge):

    def following(array):
        return jnp.roll(array, -1, axis=0)
    items = (mps, ket, left_proj, following(right_proj), bond_charge, following(bond_charge), new_charge, following(new_charge), link_charge, following(link_charge), vert_charge)

    def single(item):
        return absorb(*item)
    image = lax.map(single, items)
    count = CHI * D * D * CHI
    meansq = lax.optimization_barrier(jnp.sum(image * image, axis=(1, 2, 3, 4))) / count
    scale = lax.rsqrt(meansq + 1e-06)
    new_mps = (image * scale[:, None, None, None, None]).astype(jnp.bfloat16)
    log_norm = jnp.mean(0.5 * jnp.log(meansq + 1e-06))
    return (new_mps, log_norm)
```

```python
import jax
import jax.numpy as jnp
from jax import lax
from jax.sharding import PartitionSpec as P


def from_behind(x, axis, by):
    count = lax.axis_size(axis)
    return lax.ppermute(x, axis, [(i, (i + by) % count) for i in range(count)])


def absorb(
    mps_site,
    ket_site,
    left_site,
    right_site,
    charge_here,
    charge_next,
    fresh_here,
    fresh_next,
    link_here,
    link_next,
    vertical,
):
    upper = vertical[0]
    lower = vertical[1]
    physical = jnp.arange(ket_site.shape[4], dtype=jnp.int32)
    keep_mps = (
        charge_here[:, None, None, None] + upper[None, :, None, None] - upper[None, None, :, None]
        == charge_next[None, None, None, :]
    )
    masked_mps = jnp.where(keep_mps, mps_site, jnp.zeros_like(mps_site))
    keep_ket = (
        upper[:, None, None, None, None] + link_here[None, :, None, None, None]
        == lower[None, None, :, None, None]
        + link_next[None, None, None, :, None]
        + physical[None, None, None, None, :]
    )
    masked_ket = jnp.where(keep_ket, ket_site, jnp.zeros_like(ket_site))
    keep_left = (
        fresh_here[:, None, None, None]
        == charge_here[None, :, None, None]
        + link_here[None, None, :, None]
        - link_here[None, None, None, :]
    )
    masked_left = jnp.where(keep_left, left_site, jnp.zeros_like(left_site))
    keep_right = (
        charge_next[:, None, None, None]
        + link_next[None, :, None, None]
        - link_next[None, None, :, None]
        == fresh_next[None, None, None, :]
    )
    masked_right = jnp.where(keep_right, right_site, jnp.zeros_like(right_site))
    first = jnp.einsum(
        "xalm,auvb->xlmuvb", masked_left, masked_mps, preferred_element_type=jnp.float32
    ).astype(jnp.bfloat16)
    second = jnp.einsum(
        "xlmuvb,uldrp->xmvbdrp", first, masked_ket, preferred_element_type=jnp.float32
    ).astype(jnp.bfloat16)
    third = jnp.einsum(
        "xmvbdrp,vmesp->xbdres", second, masked_ket, preferred_element_type=jnp.float32
    ).astype(jnp.bfloat16)
    return jnp.einsum("xbdres,brsy->xdey", third, masked_right, preferred_element_type=jnp.float32)


def local(mps, ket, left_proj, right_proj, bond_charge, new_charge, link_charge, vert_charge):
    sites_here = mps.shape[0]
    half = left_proj.shape[1]
    full_mps = lax.all_gather(mps, "sec", axis=1, tiled=True)
    chi_full = full_mps.shape[1]
    legs = full_mps.shape[2]
    chi = bond_charge.shape[1]
    packed = jnp.concatenate([bond_charge, new_charge, link_charge], axis=1)
    shifted = from_behind(packed, "col", -1)
    received = (shifted[:, :chi], shifted[:, chi : 2 * chi], shifted[:, 2 * chi :])
    bond_next = jnp.concatenate([bond_charge[1:], received[0]], axis=0)
    fresh_next = jnp.concatenate([new_charge[1:], received[1]], axis=0)
    link_next = jnp.concatenate([link_charge[1:], received[2]], axis=0)
    arrived = from_behind(right_proj, "col", -1)
    partial_next = jnp.concatenate([right_proj[1:], arrived], axis=0)
    right_next = lax.all_gather(partial_next, "sec", axis=4, tiled=True)
    offset = lax.axis_index("sec") * half
    fresh_half = lax.dynamic_slice_in_dim(new_charge[0], offset, half, 0)
    images = [
        absorb(
            full_mps[0],
            ket[0],
            left_proj[0],
            right_next[0],
            bond_charge[0],
            bond_next[0],
            fresh_half,
            fresh_next[0],
            link_charge[0],
            link_next[0],
            vert_charge[0],
        )
    ]
    image = jnp.stack(images, axis=0)
    partial_value = jnp.sum(image * image)
    count = chi_full * legs * legs * chi_full
    columns = lax.axis_size("col")
    sections = lax.axis_size("sec")
    outgoing = jnp.broadcast_to(partial_value, (columns * sections, 1, 128))
    incoming = lax.all_to_all(outgoing, ("col", "sec"), 0, 0, tiled=True)
    squares = jnp.sum(incoming[:, 0, 0].reshape(columns, sections), axis=1)
    meansq_all = squares / count
    log_norm = jnp.sum(0.5 * jnp.log(meansq_all + 1e-06)) / (sites_here * columns)
    meansq = lax.dynamic_slice_in_dim(meansq_all, lax.axis_index("col"), 1, 0)
    scale = lax.rsqrt(meansq + 1e-06)
    new_mps = (image * scale[:, None, None, None, None]).astype(jnp.bfloat16)
    return (new_mps, log_norm)


def solution(mesh):
    placed = (
        P("col", "sec", None, None, None),
        P("col", None, None, None, None, None),
        P("col", "sec", None, None, None),
        P("col", None, None, None, "sec"),
        P("col", None),
        P("col", None),
        P("col", None),
        P("col", None, None),
    )
    return jax.shard_map(
        local,
        mesh=mesh,
        in_specs=placed,
        out_specs=(P("col", "sec", None, None, None), P()),
        check_vma=False,
    )
```

```python
import functools

import jax
import jax.numpy as jnp
import numpy as np
from jax import lax
from jax.experimental import pallas as pl
from jax.experimental.pallas import tpu as pltpu
from jax.sharding import PartitionSpec as P

LANES = 128
XBLOCK = 8


def round_up(value, multiple):
    return -(-value // multiple) * multiple


def from_behind(x, axis, by):
    count = lax.axis_size(axis)
    return lax.ppermute(x, axis, [(i, (i + by) % count) for i in range(count)])


class Plan:
    def __init__(self, chi, half, legs, phys):
        self.chi, self.half, self.legs, self.phys = chi, half, legs, phys
        self.lanes = round_up(chi, LANES)
        self.lm = round_up(legs * legs, 8)
        self.pairs = legs // 2
        self.group_rows = 2 * legs * phys
        self.groups = legs * self.pairs
        self.rows2 = self.groups * self.group_rows
        self.cols2 = round_up(legs * self.lm, 256)
        self.seg = round_up(2 * legs, 16)
        self.rows3 = legs * self.seg
        self.cols3 = legs * self.group_rows
        self.xrows = self.pairs * self.seg

    def matrices(self):
        n, ph = self.legs, self.phys
        r2 = np.zeros((self.rows2, n * n * ph), np.float32)
        c2 = np.zeros((n * n, self.cols2), np.float32)
        m2 = np.zeros((self.rows2, self.cols2), np.float32)
        col_m = np.full((self.cols2,), -1)
        for u in range(n):
            for l in range(n):
                for m in range(n):
                    c = u * self.lm + l * n + m
                    c2[u * n + l, c] = 1
                    col_m[c] = m
        row_m = np.zeros((self.rows2,), np.int64)
        for r in range(n):
            for d in range(n):
                for m in range(n):
                    for p in range(ph):
                        g = r * self.pairs + d // 2
                        row = g * self.group_rows + (d % 2) * n * ph + m * ph + p
                        r2[row, (d * n + r) * ph + p] = 1
                        row_m[row] = m
        m2[:] = row_m[:, None] == col_m[None, :]
        r3 = np.zeros((self.rows3, n * n), np.float32)
        c3 = np.zeros((n * n * ph, self.cols3), np.float32)
        row_d = np.full((self.rows3,), -1)
        for s in range(n):
            for d2 in range(2):
                for e in range(n):
                    row = s * self.seg + d2 * n + e
                    r3[row, e * n + s] = 1
                    row_d[row] = d2
        col_d = np.zeros((self.cols3,), np.int64)
        for v in range(n):
            for d2 in range(2):
                for m in range(n):
                    for p in range(ph):
                        col = v * self.group_rows + d2 * n * ph + m * ph + p
                        c3[(v * n + m) * ph + p, col] = 1
                        col_d[col] = d2
        m3 = (row_d[:, None] == col_d[None, :]).astype(np.float32)
        as_bf16 = lambda x: jnp.asarray(x, jnp.bfloat16)
        return [as_bf16(x) for x in (r2, c2, m2, r3, c3, m3)]

    def indices(self):
        n, ph = self.legs, self.phys
        count = n * n * ph
        rows = np.zeros((count, 8), np.int32)
        cols = np.zeros((8, count), np.int32)
        for i in range(count):
            hi, mid, p = i // (n * ph), (i // ph) % n, i % ph
            rows[i, :3] = hi, mid, p
            cols[:3, i] = hi, mid, p
            if i < n * n:
                rows[i, 3:5] = i // n, i % n
                cols[3:5, i] = i // n, i % n
        return jnp.asarray(rows), jnp.asarray(cols)


def look_up(index, table):
    out = jnp.zeros(index.shape, jnp.int32)
    for k, value in enumerate(table):
        out = out + jnp.where(index == k, value, 0)
    return out


def dot(a, b):
    return jnp.dot(a, b, preferred_element_type=jnp.float32)


def absorb_kernel(
    plan,
    next_s,
    own_s,
    next_v,
    bond_col,
    mine,
    other,
    lhs,
    ket_a,
    ket_b,
    r2,
    c2,
    m2,
    r3,
    c3,
    m3,
    rows,
    cols,
    pr_mine,
    pr_other,
    image,
    partial,
    ms,
    k2,
    k3,
    pr,
    w1,
    w2,
    w3,
):
    n, ph, chi, half = plan.legs, plan.phys, plan.chi, plan.half
    lanes, lm, gr = plan.lanes, plan.lm, plan.group_rows
    step = pl.program_id(0)
    bf16 = jnp.bfloat16

    @pl.when(step == 0)
    def _():
        sec = lax.axis_index("sec")
        link = [own_s[0, i] for i in range(n)]
        upper = [own_s[0, n + i] for i in range(n)]
        lower = [own_s[0, 2 * n + i] for i in range(n)]
        link_next = [next_s[0, 2 * chi + i] for i in range(n)]
        bond_next = next_v[:, :chi]
        ms[...] = jnp.zeros_like(ms)
        for k, src in enumerate((mine, other)):
            which = sec if k == 0 else 1 - sec
            at = pl.multiple_of(which * half, 16)
            gap = bond_next - bond_col[pl.ds(at, half), :]
            for u in range(n):
                for v in range(n):
                    keep = gap == upper[u] - upper[v]
                    val = jnp.where(keep, src[u * n + v].astype(jnp.float32), 0.0)
                    ms[u, v // 2, pl.ds(at, half), (v % 2) * lanes : (v % 2) * lanes + chi] = val.astype(bf16)
        row_a = look_up(rows[:, 0:1], lower) + look_up(rows[:, 1:2], link_next) + rows[:, 2:3]
        col_a = look_up(cols[3:4, : n * n], upper) + look_up(cols[4:5, : n * n], link)
        kept_a = jnp.where(row_a == col_a, ket_a[...].astype(jnp.float32), 0.0).astype(bf16)
        wide = dot(dot(r2[...], kept_a).astype(bf16), c2[...])
        k2[...] = (wide * m2[...].astype(jnp.float32)).astype(bf16)
        row_b = look_up(rows[: n * n, 3:4], lower) + look_up(rows[: n * n, 4:5], link_next)
        col_b = look_up(cols[0:1, :], upper) + look_up(cols[1:2, :], link) - cols[2:3, :]
        kept_b = jnp.where(row_b == col_b, ket_b[...].astype(jnp.float32), 0.0).astype(bf16)
        wide = dot(dot(r3[...], kept_b).astype(bf16), c3[...])
        k3[...] = (wide * m3[...].astype(jnp.float32)).astype(bf16)
        square = (chi, chi)
        diagonal = lax.broadcasted_iota(jnp.int32, square, 0) == lax.broadcasted_iota(jnp.int32, square, 1)
        fresh_row = jnp.broadcast_to(next_v[:, chi : 2 * chi], square)
        fresh_col = jnp.sum(jnp.where(diagonal, fresh_row, 0), axis=1, keepdims=True)
        gap_low = fresh_col[:half] - bond_next
        gap_high = fresh_col[half:] - bond_next
        pr[...] = jnp.zeros_like(pr)
        for k, src in enumerate((pr_mine, pr_other)):
            which = sec if k == 0 else 1 - sec
            at = pl.multiple_of(which * half, 16)
            gap = jnp.where(which == 0, gap_low, gap_high)
            for r in range(n):
                for s in range(n):
                    keep = gap == link_next[r] - link_next[s]
                    val = jnp.where(keep, src[r * n + s].astype(jnp.float32), 0.0)
                    pr[r, pl.ds(at, half), s * lanes : s * lanes + chi] = val.astype(bf16)
        w1[...] = jnp.zeros_like(w1)
        partial[...] = jnp.zeros_like(partial)

    for q in range(XBLOCK // 2):
        slot = q % 2
        left = lhs[q * 2 * lm : (q + 1) * 2 * lm, :]
        for vp in range(plan.pairs):
            for up in range(plan.pairs):
                lo = dot(left, ms[2 * up, vp])
                hi = dot(left, ms[2 * up + 1, vp])
                for x in range(2):
                    both = jnp.concatenate([lo[x * lm : (x + 1) * lm], hi[x * lm : (x + 1) * lm]], axis=0)
                    w1[slot, x, vp, up * 2 * lm : (up + 1) * 2 * lm, :] = both.astype(bf16)
            for x in range(2):
                out = dot(k2[...], w1[slot, x, vp])
                for g in range(plan.groups):
                    part = out[g * gr : (g + 1) * gr]
                    both = jnp.concatenate([part[:, :lanes], part[:, lanes:]], axis=0)
                    w2[slot, g, vp * 2 * gr : (vp + 1) * 2 * gr, x * lanes : (x + 1) * lanes] = both.astype(bf16)
        for g in range(plan.groups):
            r, dp = g // plan.pairs, g % plan.pairs
            out = dot(k3[...], w2[slot, g]).astype(bf16)
            for s in range(n):
                for x in range(2):
                    at = (q * 2 + x) * plan.xrows + dp * plan.seg
                    w3[r, at : at + plan.seg, s * lanes : (s + 1) * lanes] = out[
                        s * plan.seg : (s + 1) * plan.seg, x * lanes : (x + 1) * lanes
                    ]
    total = None
    for r in range(n):
        term = lax.dot_general(w3[r], pr[r], (((1,), (1,)), ((), ())), preferred_element_type=jnp.float32)
        total = term if total is None else total + term
    image[...] = total
    partial[...] += jnp.sum(total * total)


def absorb(plan, next_all, own_s, bond_col, mine, other, lhs, ket, pr_mine, pr_other):
    n, ph, chi, half = plan.legs, plan.phys, plan.chi, plan.half
    ket_a = jnp.transpose(ket, (2, 3, 4, 0, 1)).reshape(n * n * ph, n * n)
    ket_b = jnp.transpose(ket, (2, 3, 0, 1, 4)).reshape(n * n, n * n * ph)
    steps = half // XBLOCK
    block = XBLOCK * plan.xrows
    operands = [next_all, own_s, next_all, bond_col, mine, other, lhs, ket_a, ket_b]
    operands += plan.matrices() + list(plan.indices()) + [pr_mine, pr_other]
    specs = []
    for i, x in enumerate(operands):
        if i < 2:
            specs.append(pl.BlockSpec(memory_space=pltpu.SMEM))
        elif i == 6:
            specs.append(pl.BlockSpec((XBLOCK * plan.lm, chi), lambda i: (i, 0)))
        else:
            specs.append(pl.BlockSpec(x.shape, functools.partial(lambda nd, i: (0,) * nd, x.ndim)))
    bf16 = jnp.bfloat16
    return pl.pallas_call(
        functools.partial(absorb_kernel, plan),
        grid=(steps,),
        in_specs=specs,
        out_specs=[
            pl.BlockSpec((block, chi), lambda i: (i, 0)),
            pl.BlockSpec((8, LANES), lambda i: (0, 0)),
        ],
        out_shape=[
            jax.ShapeDtypeStruct((half * plan.xrows, chi), jnp.float32),
            jax.ShapeDtypeStruct((8, LANES), jnp.float32),
        ],
        scratch_shapes=[
            pltpu.VMEM((n, plan.pairs, chi, 2 * plan.lanes), bf16),
            pltpu.VMEM((plan.rows2, plan.cols2), bf16),
            pltpu.VMEM((plan.rows3, plan.cols3), bf16),
            pltpu.VMEM((n, chi, n * plan.lanes), bf16),
            pltpu.VMEM((2, 2, plan.pairs, plan.cols2, 2 * plan.lanes), bf16),
            pltpu.VMEM((2, plan.groups, plan.cols3, 2 * plan.lanes), bf16),
            pltpu.VMEM((n, block, n * plan.lanes), bf16),
        ],
        name="absorb",
    )(*operands)


def local(mps, ket, left_proj, right_proj, bond_charge, new_charge, link_charge, vert_charge):
    half, chi, legs = left_proj.shape[1], left_proj.shape[2], left_proj.shape[3]
    phys = ket.shape[5]
    plan = Plan(chi, half, legs, phys)
    columns, sections = lax.axis_size("col"), lax.axis_size("sec")
    swap = [(i, 1 - i) for i in range(sections)]
    packed = jnp.concatenate([bond_charge, new_charge, link_charge], axis=1)
    next_all = from_behind(packed, "col", -1)
    mine = jnp.transpose(mps[0], (1, 2, 0, 3)).reshape(legs * legs, half, chi)
    other = lax.ppermute(mine, "sec", swap)
    pr_mine = from_behind(jnp.transpose(right_proj[0], (1, 2, 3, 0)).reshape(legs * legs, half, chi), "col", -1)
    pr_other = lax.ppermute(pr_mine, "sec", swap)
    sec = lax.axis_index("sec")
    fresh = lax.dynamic_slice_in_dim(new_charge[0], sec * half, half, 0)
    link = link_charge[0]
    keep = (
        fresh[None, None, :, None]
        == bond_charge[0][None, None, None, :] + link[:, None, None, None] - link[None, :, None, None]
    )
    left = jnp.transpose(left_proj[0], (2, 3, 0, 1))
    left = jnp.where(keep, left, jnp.zeros_like(left)).reshape(legs * legs, half, chi)
    left = jnp.transpose(left, (1, 0, 2))
    left = jnp.pad(left, ((0, 0), (0, plan.lm - legs * legs), (0, 0))).reshape(half * plan.lm, chi)
    own_s = jnp.concatenate([link_charge, vert_charge[:, 0], vert_charge[:, 1]], axis=1)
    image, partial = absorb(
        plan, next_all, own_s, bond_charge[0][:, None], mine, other, left, ket[0], pr_mine, pr_other
    )
    count = chi * legs * legs * chi
    outgoing = jnp.broadcast_to(partial[:1], (columns * sections, 1, LANES))
    incoming = lax.all_to_all(outgoing, ("col", "sec"), 0, 0, tiled=True)
    squares = jnp.sum(incoming[:, 0, 0].reshape(columns, sections), axis=1)
    meansq_all = squares / count
    log_norm = jnp.sum(0.5 * jnp.log(meansq_all + 1e-06)) / columns
    meansq = lax.dynamic_slice_in_dim(meansq_all, lax.axis_index("col"), 1, 0)
    scale = lax.rsqrt(meansq + 1e-06)[0]
    shaped = image.reshape(half, plan.pairs, plan.seg, chi)[:, :, : 2 * legs].reshape(half, legs, legs, chi)
    new_mps = (shaped * scale).astype(jnp.bfloat16)[None]
    return (new_mps, log_norm)


def solution(mesh):
    placed = (
        P("col", "sec", None, None, None),
        P("col", None, None, None, None, None),
        P("col", "sec", None, None, None),
        P("col", None, None, None, "sec"),
        P("col", None),
        P("col", None),
        P("col", None),
        P("col", None, None),
    )
    return jax.shard_map(
        local,
        mesh=mesh,
        in_specs=placed,
        out_specs=(P("col", "sec", None, None, None), P()),
        check_vma=False,
    )
```

```python
import functools

import jax
import jax.numpy as jnp
import numpy as np
from jax import lax
from jax.experimental import pallas as pl
from jax.experimental.pallas import tpu as pltpu
from jax.sharding import PartitionSpec as P

LANES = 128
QUAD = 4
VMEM_LIMIT = 36 << 20
FRONT_FLOPS = 1 << 30


def round_up(value, multiple):
    return -(-value // multiple) * multiple


def from_behind(x, axis, by):
    count = lax.axis_size(axis)
    return lax.ppermute(x, axis, [(i, (i + by) % count) for i in range(count)])


class Plan:
    def __init__(self, chi, half, legs, phys):
        self.chi, self.half, self.legs, self.phys = chi, half, legs, phys
        self.lanes = round_up(chi, LANES)
        self.lm = round_up(legs * legs, 8)
        self.pairs = legs // 2
        self.group_rows = 2 * legs * phys
        self.groups = legs * self.pairs
        self.rows2 = self.groups * self.group_rows
        self.cols2 = round_up(legs * self.lm, 256)
        self.seg = round_up(2 * legs, 16)
        self.rows3 = legs * self.seg
        self.cols3 = legs * self.group_rows
        self.xrows = self.pairs * self.seg

    def matrices(self):
        n, ph = self.legs, self.phys
        wide = n * n * ph
        r2 = np.zeros((self.rows2, wide), np.float32)
        row_m = np.zeros((self.rows2,), np.int64)
        for r in range(n):
            for d in range(n):
                for m in range(n):
                    for p in range(ph):
                        g = r * self.pairs + d // 2
                        row = g * self.group_rows + (d % 2) * n * ph + m * ph + p
                        r2[row, (d * ph + p) * n + r] = 1
                        row_m[row] = m
        c2 = np.zeros((n * n, self.cols2), np.float32)
        col_m = np.full((self.cols2,), -1)
        for u in range(n):
            for l in range(n):
                for m in range(n):
                    c = u * self.lm + l * n + m
                    c2[u * n + l, c] = 1
                    col_m[c] = m
        m2 = row_m[:, None] == col_m[None, :]
        r3 = np.zeros((ph, self.rows3, wide), np.float32)
        row_d = np.full((self.rows3,), -1)
        for s in range(n):
            for d2 in range(2):
                for e in range(n):
                    row = s * self.seg + d2 * n + e
                    row_d[row] = d2
                    for p in range(ph):
                        r3[p, row, (e * ph + p) * n + s] = 1
        c3 = np.zeros((ph, n * n, self.cols3), np.float32)
        col_d = np.zeros((self.cols3,), np.int64)
        for v in range(n):
            for d2 in range(2):
                for m in range(n):
                    for p in range(ph):
                        col = v * self.group_rows + d2 * n * ph + m * ph + p
                        c3[p, v * n + m, col] = 1
                        col_d[col] = d2
        m3 = row_d[:, None] == col_d[None, :]
        return [jnp.asarray(x, jnp.bfloat16) for x in (r2, c2, m2, r3, c3, m3)]

    def indices(self):
        n, ph = self.legs, self.phys
        rows = np.zeros((n * n * ph, 8), np.int32)
        cols = np.zeros((8, self.cols2), np.int32)
        for i in range(n * n * ph):
            rest = i % self.group_rows
            rows[i, 0] = i // self.group_rows * 2 + rest // (n * ph)
            rows[i, 1] = rest % ph
        for i in range(self.seg):
            rows[i, 2] = i % n
        for u in range(n):
            for i in range(n * n):
                cols[:2, u * self.lm + i] = u, i // n
        for i in range(self.cols3):
            rest = i % (n * ph)
            cols[2:5, i] = i // self.group_rows, rest // ph, rest % ph
        return [jnp.asarray(rows), jnp.asarray(cols)]


def column_of(row):
    square = (row.shape[1], row.shape[1])
    diagonal = lax.broadcasted_iota(jnp.int32, square, 0) == lax.broadcasted_iota(jnp.int32, square, 1)
    return jnp.sum(jnp.where(diagonal, jnp.broadcast_to(row, square), 0), axis=1, keepdims=True)


def look_up(index, table):
    out = jnp.zeros(index.shape, jnp.int32)
    for k, value in enumerate(table):
        out = out + jnp.where(index == k, value, 0)
    return out


def dot(a, b):
    return jnp.dot(a, b, preferred_element_type=jnp.float32)


def fetch(pairs, sems):
    copies = [pltpu.make_async_copy(src, dst, sems.at[i]) for i, (src, dst) in enumerate(pairs)]
    for copy in copies:
        copy.start()
    return copies


def prep_kernel(
    plan,
    ket, left_h, bond_h, fresh_h, link_h, vert_h, r2_h, c2_h, m2_h, r3_h, c3_h, m3_h, rows_h, cols_h,
    out, k2, k3, gap2, gap3, bond_col,
    wide, left, bond, fresh, link_s, vert_s, r2, c2, m2, r3, c3, m3, rows, cols, sems,
):
    n, half, lm = plan.legs, plan.half, plan.lm
    sources = (link_h, vert_h, bond_h, fresh_h, left_h, r2_h, c2_h, m2_h, r3_h, c3_h, m3_h, rows_h, cols_h)
    targets = (link_s, vert_s, bond, fresh, left, r2, c2, m2, r3, c3, m3, rows, cols)
    copies = fetch(list(zip(sources, targets)), sems)
    for row in range(n * n, lm):
        wide[pl.ds(row, half, stride=lm), :] = jnp.zeros((half, plan.chi), jnp.float32)
    for copy in copies[:5]:
        copy.wait()
    sec = lax.axis_index("sec")
    link = [link_s[0, i] for i in range(n)]
    upper = [vert_s[0, 0, i] for i in range(n)]
    lower = [vert_s[0, 1, i] for i in range(n)]
    fresh_all = column_of(fresh[...])
    fresh_col = jnp.where(sec == 0, fresh_all[:half], fresh_all[half:])
    bond_col[...] = column_of(bond[...])
    gap = fresh_col - bond[...]
    for l in range(n):
        for m in range(n):
            keep = gap == link[l] - link[m]
            val = jnp.where(keep, left[l * n + m].astype(jnp.float32), 0.0)
            wide[pl.ds(l * n + m, half, stride=lm), :] = val
    out[...] = wide[...].astype(jnp.bfloat16)
    for copy in copies[5:]:
        copy.wait()

    def expand(first, second):
        picked = lax.dot_general(first, ket[...], (((1,), (1,)), ((), ())), preferred_element_type=jnp.float32)
        return dot(picked.astype(jnp.bfloat16), second)

    k2[...] = (expand(r2[...], c2[...]) * m2[...].astype(jnp.float32)).astype(jnp.bfloat16)
    total = expand(r3[0], c3[0])
    for p in range(1, plan.phys):
        total = total + expand(r3[p], c3[p])
    k3[...] = (total * m3[...].astype(jnp.float32)).astype(jnp.bfloat16)
    rows_d = look_up(rows[:, 0:1], lower) + rows[:, 1:2]
    gap2[...] = look_up(cols[0:1, :], upper) + look_up(cols[1:2, :], link) - rows_d
    rows_e = look_up(rows[: plan.seg, 2:3], lower)
    c = slice(0, plan.cols3)
    gap3[...] = look_up(cols[2:3, c], upper) + look_up(cols[3:4, c], link) - cols[4:5, c] - rows_e


def halves(first, second):
    sec = lax.axis_index("sec")
    return ((first, sec), (second, 1 - sec))


def first_two(plan, left, ms, k2, w1, w2, vp):
    lanes, lm, gr = plan.lanes, plan.lm, plan.group_rows
    bf16 = jnp.bfloat16
    for up in range(plan.pairs):
        both = dot(left, ms[up, vp])
        for x in range(QUAD):
            part = both[x * lm : (x + 1) * lm]
            stacked = jnp.concatenate([part[:, : 2 * lanes], part[:, 2 * lanes :]], axis=0)
            w1[vp, up * 2 * lm : (up + 1) * 2 * lm, x * 2 * lanes : (x + 1) * 2 * lanes] = stacked.astype(bf16)
    for h in range(QUAD // 2):
        out = dot(k2[...], w1[vp, :, h * 4 * lanes : (h + 1) * 4 * lanes])
        for g in range(plan.groups):
            part = out[g * gr : (g + 1) * gr]
            for j in range(2):
                x = 2 * h + j
                low, high = part[:, 2 * j * lanes : (2 * j + 1) * lanes], part[:, (2 * j + 1) * lanes : (2 * j + 2) * lanes]
                stacked = jnp.concatenate([low, high], axis=0)
                w2[g, vp * 2 * gr : (vp + 1) * 2 * gr, x * lanes : (x + 1) * lanes] = stacked.astype(bf16)


def third(plan, k3, w2, w3, g):
    lanes, seg = plan.lanes, plan.seg
    r, dp = g // plan.pairs, g % plan.pairs
    out = dot(k3[...], w2[g]).astype(jnp.bfloat16)
    for s in range(plan.legs):
        for x in range(QUAD):
            at = x * plan.xrows + dp * seg
            w3[r, at : at + seg, s * lanes : (s + 1) * lanes] = out[s * seg : (s + 1) * seg, x * lanes : (x + 1) * lanes]


def fourth(w3, pr, r):
    return lax.dot_general(w3[r], pr[r], (((1,), (1,)), ((), ())), preferred_element_type=jnp.float32)


def add(total, term):
    return term if total is None else total + term


def quad_rows(lhs, plan, quad):
    rows = QUAD * plan.lm
    return lhs[pl.ds(pl.multiple_of(quad * rows, 16), rows), :]


def front_kernel(
    plan, ahead,
    link_next_s, bond_next_v, other, lhs, k2_all, k3_all, gap2, gap3, bond_col, mine_h, vert_h,
    ms, k2, k3, w3,
    w1, w2, mine, vert_s, sems,
):
    n, chi, half, lanes = plan.legs, plan.chi, plan.half, plan.lanes
    bf16 = jnp.bfloat16
    copies = fetch([(vert_h, vert_s), (mine_h, mine)], sems)
    link_next = [link_next_s[0, i] for i in range(n)]
    tall = plan.pairs * plan.group_rows
    for r in range(n):
        at = slice(r * tall, (r + 1) * tall)
        k2[at] = jnp.where(gap2[...] == link_next[r], k2_all[at].astype(jnp.float32), 0.0).astype(bf16)
        at = slice(r * plan.seg, (r + 1) * plan.seg)
        k3[at] = jnp.where(gap3[...] == link_next[r], k3_all[at].astype(jnp.float32), 0.0).astype(bf16)
    if chi < lanes:
        for k in range(4):
            at = slice(k * lanes + chi, (k + 1) * lanes)
            ms[:, :, :, at] = jnp.zeros((plan.pairs, plan.pairs, chi, lanes - chi), bf16)
    copies[0].wait()
    upper = [vert_s[0, 0, i] for i in range(n)]
    copies[1].wait()
    for src, which in halves(mine, other):
        at = pl.multiple_of(which * half, 16)
        gap = bond_next_v[...] - bond_col[pl.ds(at, half), :]
        for u in range(n):
            for v in range(n):
                keep = gap == upper[u] - upper[v]
                val = jnp.where(keep, src[u * n + v].astype(jnp.float32), 0.0)
                lane = (u % 2 * 2 + v % 2) * lanes
                ms[u // 2, v // 2, pl.ds(at, half), lane : lane + chi] = val.astype(bf16)
    pad = n * plan.lm
    w1[:, :, pad:, :] = jnp.zeros((2, plan.pairs, plan.cols2 - pad, w1.shape[3]), bf16)
    per_g = plan.groups // plan.pairs
    for q in range(ahead + 1):
        for vp in range(plan.pairs):
            if q < ahead:
                first_two(plan, quad_rows(lhs, plan, q), ms, k2, w1.at[q % 2], w2.at[q % 2], vp)
            if q > 0:
                for g in range(vp * per_g, (vp + 1) * per_g):
                    third(plan, k3, w2.at[(q - 1) % 2], w3.at[q - 1], g)


def back_kernel(
    plan, ahead,
    link_next_s,
    bond_next_v, fresh_next_v, lhs, ms, k2, k3, w3_ahead, pr_mine, pr_other,
    image, partial,
    pr, w1, w2, w3,
):
    n, chi, half, lanes = plan.legs, plan.chi, plan.half, plan.lanes
    bf16 = jnp.bfloat16
    link_next = [link_next_s[0, i] for i in range(n)]
    fresh_col = column_of(fresh_next_v[...])
    pr[...] = jnp.zeros_like(pr)
    for src, which in halves(pr_mine, pr_other):
        at = pl.multiple_of(which * half, 16)
        gap = jnp.where(which == 0, fresh_col[:half], fresh_col[half:]) - bond_next_v[...]
        for r in range(n):
            for s in range(n):
                keep = gap == link_next[r] - link_next[s]
                val = jnp.where(keep, src[r * n + s].astype(jnp.float32), 0.0)
                pr[r, pl.ds(at, half), s * lanes : s * lanes + chi] = val.astype(bf16)
    pad = n * plan.lm
    w1[:, :, pad:, :] = jnp.zeros((2, plan.pairs, plan.cols2 - pad, w1.shape[3]), bf16)

    block = QUAD * plan.xrows
    per_g = plan.groups // plan.pairs
    per_r = n // plan.pairs

    def put(quad, total):
        image[pl.ds(pl.multiple_of(quad * block, 8), block), :] = total
        return jnp.sum(total * total)

    def body(step, square_sum):
        early = None
        for k in range(2):
            total = None
            for vp in range(plan.pairs):
                left = quad_rows(lhs, plan, ahead + 2 * step + k)
                first_two(plan, left, ms, k2, w1.at[k], w2.at[k], vp)
                for g in range(vp * per_g, (vp + 1) * per_g):
                    third(plan, k3, w2.at[1 - k], w3.at[1 - k], g)
                for r in range(vp * per_r, (vp + 1) * per_r):
                    total = add(total, fourth(w3.at[k], pr, r))
                    if r % 2 == k:
                        early = add(early, fourth(w3_ahead.at[step], pr, r))
            square_sum = square_sum + jnp.where(step > 0, put(ahead - 2 + 2 * step + k, total), 0.0)
        return square_sum + put(step, early)

    quads = half // QUAD
    steps = (quads - ahead) // 2
    square_sum = lax.fori_loop(0, steps, body, jnp.float32(0.0))
    total = None
    for g in range(plan.groups):
        third(plan, k3, w2.at[1], w3.at[1], g)
        if g % plan.pairs == 0:
            total = add(total, fourth(w3.at[0], pr, g // plan.pairs))
    square_sum = square_sum + put(quads - 2, total)
    even = odd = None
    for r in range(0, n, 2):
        even = add(even, fourth(w3.at[1], pr, r))
        odd = add(odd, fourth(w3.at[1], pr, r + 1))
    square_sum = square_sum + put(quads - 1, even + odd)
    partial[...] = jnp.full_like(partial, square_sum)


def finish_kernel(plan, count, columns, incoming, image, new, log_norm):
    n, half = plan.legs, plan.half
    sums = incoming[...]
    devices = sums.shape[0]
    row = lax.broadcasted_iota(jnp.int32, sums.shape, 0)
    pair = sums + pltpu.roll(sums, devices - 1, 0)
    logs = 0.5 * jnp.log(pair / count + 1e-06)
    log_norm[0, 0] = jnp.sum(jnp.where(row % 2 == 0, logs, 0.0)[:, :1]) / columns
    here = jnp.sum(jnp.where(row == 2 * lax.axis_index("col"), pair, 0.0), axis=0, keepdims=True)
    scale = lax.rsqrt(here / count + 1e-06)[:, : plan.chi]
    for d in range(n):
        for e in range(n):
            at = (d // 2) * plan.seg + (d % 2) * n + e
            new[d * n + e] = (image[pl.ds(at, half, stride=plan.xrows), :] * scale).astype(jnp.bfloat16)


def whole(memory, count):
    return [pl.BlockSpec(memory_space=memory) for _ in range(count)]


def absorb_row(mps, ket, left_proj, right_proj, bond_charge, new_charge, link_charge, vert_charge):
    half, chi, legs = left_proj.shape[1], left_proj.shape[2], left_proj.shape[3]
    phys = ket.shape[5]
    plan = Plan(chi, half, legs, phys)
    squared = legs * legs
    columns, sections = lax.axis_size("col"), lax.axis_size("sec")
    bf16, f32 = jnp.bfloat16, jnp.float32
    smem, vmem = pltpu.SMEM, pltpu.VMEM
    swap = [(i, 1 - i) for i in range(sections)]
    hbm = pltpu.HBM
    bond_next, fresh_next, link_next = from_behind((bond_charge, new_charge, link_charge), "col", -1)
    mine = jnp.transpose(mps[0], (1, 2, 0, 3)).reshape(squared, half, chi)
    other = lax.ppermute(mine, "sec", swap)
    pr_mine = from_behind(jnp.transpose(right_proj[0], (1, 2, 3, 0)).reshape(squared, half, chi), "col", -1)
    bond_next, fresh_next, link_next = lax.optimization_barrier((bond_next, fresh_next, link_next))
    left = jnp.transpose(left_proj[0], (2, 3, 0, 1)).reshape(squared, half, chi)
    flat_ket = jnp.transpose(ket[0], (0, 1, 2, 4, 3)).reshape(squared, squared * phys)
    fetched = [left, bond_charge, new_charge, link_charge, vert_charge] + plan.matrices() + plan.indices()
    in_smem = (3, 4)
    scratch = [(smem if i in in_smem else vmem)(x.shape, x.dtype) for i, x in enumerate(fetched)]
    scratch = [scratch[i] for i in (0, 1, 2, 3, 4)] + scratch[5:]
    lhs, *kets = pl.pallas_call(
        functools.partial(prep_kernel, plan),
        in_specs=whole(vmem, 1) + whole(hbm, len(fetched)),
        out_specs=whole(vmem, 6),
        out_shape=[
            jax.ShapeDtypeStruct((half * plan.lm, chi), bf16),
            jax.ShapeDtypeStruct((plan.rows2, plan.cols2), bf16),
            jax.ShapeDtypeStruct((plan.rows3, plan.cols3), bf16),
            jax.ShapeDtypeStruct((squared * phys, plan.cols2), jnp.int32),
            jax.ShapeDtypeStruct((plan.seg, plan.cols3), jnp.int32),
            jax.ShapeDtypeStruct((chi, 1), jnp.int32),
        ],
        scratch_shapes=[pltpu.VMEM((half * plan.lm, chi), f32)] + scratch + [pltpu.SemaphoreType.DMA((len(fetched),))],
        compiler_params=pltpu.CompilerParams(vmem_limit_bytes=12 << 20),
        cost_estimate=pl.CostEstimate(flops=FRONT_FLOPS // 8, bytes_accessed=1 << 20, transcendentals=0),
        name="prep",
    )(flat_ket, *[pltpu.with_memory_space_constraint(x, pltpu.HBM) for x in fetched])
    quads = half // QUAD
    ahead = quads // 3
    block = QUAD * plan.xrows
    lanes = plan.lanes
    step_scratch = [
        pltpu.VMEM((2, plan.pairs, plan.cols2, 2 * QUAD * lanes), bf16),
        pltpu.VMEM((2, plan.groups, plan.cols3, QUAD * lanes), bf16),
    ]
    operands = [link_next, bond_next, other, lhs] + kets
    operands += [pltpu.with_memory_space_constraint(x, pltpu.HBM) for x in (mine, vert_charge)]
    ms, k2, k3, w3_ahead = pl.pallas_call(
        functools.partial(front_kernel, plan, ahead),
        in_specs=whole(smem, 1) + whole(vmem, len(operands) - 3) + whole(hbm, 2),
        out_specs=whole(vmem, 4),
        out_shape=[
            jax.ShapeDtypeStruct((plan.pairs, plan.pairs, chi, 4 * lanes), bf16),
            jax.ShapeDtypeStruct((plan.rows2, plan.cols2), bf16),
            jax.ShapeDtypeStruct((plan.rows3, plan.cols3), bf16),
            jax.ShapeDtypeStruct((ahead, legs, block, legs * lanes), bf16),
        ],
        scratch_shapes=step_scratch
        + [
            pltpu.VMEM(mine.shape, bf16),
            pltpu.SMEM(vert_charge.shape, jnp.int32),
            pltpu.SemaphoreType.DMA((2,)),
        ],
        compiler_params=pltpu.CompilerParams(vmem_limit_bytes=VMEM_LIMIT),
        cost_estimate=pl.CostEstimate(flops=FRONT_FLOPS, bytes_accessed=1 << 20, transcendentals=0),
        name="front",
    )(*operands)
    pr_mine, w3_ahead = lax.optimization_barrier((pr_mine, w3_ahead))
    pr_other = lax.ppermute(pr_mine, "sec", swap)
    operands = [link_next, bond_next, fresh_next, lhs, ms, k2, k3, w3_ahead, pr_mine, pr_other]
    image, partial = pl.pallas_call(
        functools.partial(back_kernel, plan, ahead),
        in_specs=whole(smem, 1) + whole(vmem, len(operands) - 1),
        out_specs=whole(vmem, 2),
        out_shape=[
            jax.ShapeDtypeStruct((quads * block, chi), f32),
            jax.ShapeDtypeStruct((columns * sections, 1, LANES), f32),
        ],
        scratch_shapes=[pltpu.VMEM((legs, chi, legs * lanes), bf16)]
        + step_scratch
        + [pltpu.VMEM((2, legs, block, legs * lanes), bf16)],
        compiler_params=pltpu.CompilerParams(vmem_limit_bytes=VMEM_LIMIT),
        cost_estimate=pl.CostEstimate(flops=2 * FRONT_FLOPS, bytes_accessed=1 << 20, transcendentals=0),
        name="back",
    )(*operands)
    incoming = lax.all_to_all(partial, ("col", "sec"), 0, 0, tiled=True)
    new, log_norm = pl.pallas_call(
        functools.partial(finish_kernel, plan, float(chi * squared * chi), float(columns)),
        in_specs=whole(vmem, 2),
        out_specs=whole(vmem, 1) + whole(smem, 1),
        out_shape=[
            jax.ShapeDtypeStruct((squared, half, chi), bf16),
            jax.ShapeDtypeStruct((1, 1), f32),
        ],
        compiler_params=pltpu.CompilerParams(vmem_limit_bytes=8 << 20),
        name="finish",
    )(incoming.reshape(columns * sections, LANES), image)
    new_mps = jnp.transpose(new.reshape(legs, legs, half, chi), (2, 0, 1, 3))[None]
    return (new_mps, log_norm.reshape(()))


def solution(mesh):
    placed = (
        P("col", "sec", None, None, None),
        P("col", None, None, None, None, None),
        P("col", "sec", None, None, None),
        P("col", None, None, None, "sec"),
        P("col", None),
        P("col", None),
        P("col", None),
        P("col", None, None),
    )
    return jax.shard_map(
        absorb_row,
        mesh=mesh,
        in_specs=placed,
        out_specs=(P("col", "sec", None, None, None), P()),
        check_vma=False,
    )
```

```python
import functools

import jax
import jax.numpy as jnp
import numpy as np
from jax import lax
from jax.experimental import pallas as pl
from jax.experimental.pallas import tpu as pltpu
from jax.sharding import PartitionSpec as P

LANES = 128
QUAD = 4
VMEM_LIMIT = 36 << 20
FRONT_FLOPS = 1 << 30


def round_up(value, multiple):
    return -(-value // multiple) * multiple


def from_behind(x, axis, by):
    count = lax.axis_size(axis)
    return lax.ppermute(x, axis, [(i, (i + by) % count) for i in range(count)])


class Plan:
    def __init__(self, chi, half, legs, phys):
        self.chi, self.half, self.legs, self.phys = chi, half, legs, phys
        self.lanes = round_up(chi, LANES)
        self.lm = round_up(legs * legs, 8)
        self.pairs = legs // 2
        self.group_rows = 2 * legs * phys
        self.groups = legs * self.pairs
        self.rows2 = self.groups * self.group_rows
        self.cols2 = round_up(legs * self.lm, 256)
        self.seg = round_up(2 * legs, 16)
        self.rows3 = legs * self.seg
        self.cols3 = legs * self.group_rows
        self.xrows = self.pairs * self.seg

    def matrices(self):
        n, ph = self.legs, self.phys
        wide = n * n * ph
        r2 = np.zeros((self.rows2, wide), np.float32)
        row_m = np.zeros((self.rows2,), np.int64)
        for r in range(n):
            for d in range(n):
                for m in range(n):
                    for p in range(ph):
                        g = r * self.pairs + d // 2
                        row = g * self.group_rows + (d % 2) * n * ph + m * ph + p
                        r2[row, (d * ph + p) * n + r] = 1
                        row_m[row] = m
        c2 = np.zeros((n * n, self.cols2), np.float32)
        col_m = np.full((self.cols2,), -1)
        for u in range(n):
            for l in range(n):
                for m in range(n):
                    c = u * self.lm + l * n + m
                    c2[u * n + l, c] = 1
                    col_m[c] = m
        m2 = row_m[:, None] == col_m[None, :]
        r3 = np.zeros((ph, self.rows3, wide), np.float32)
        row_d = np.full((self.rows3,), -1)
        for s in range(n):
            for d2 in range(2):
                for e in range(n):
                    row = s * self.seg + d2 * n + e
                    row_d[row] = d2
                    for p in range(ph):
                        r3[p, row, (e * ph + p) * n + s] = 1
        c3 = np.zeros((ph, n * n, self.cols3), np.float32)
        col_d = np.zeros((self.cols3,), np.int64)
        for v in range(n):
            for d2 in range(2):
                for m in range(n):
                    for p in range(ph):
                        col = v * self.group_rows + d2 * n * ph + m * ph + p
                        c3[p, v * n + m, col] = 1
                        col_d[col] = d2
        m3 = row_d[:, None] == col_d[None, :]
        return [jnp.asarray(x, jnp.bfloat16) for x in (r2, c2, m2, r3, c3, m3)]

    def indices(self):
        n, ph = self.legs, self.phys
        rows = np.zeros((n * n * ph, 8), np.int32)
        cols = np.zeros((8, self.cols2), np.int32)
        for i in range(n * n * ph):
            rest = i % self.group_rows
            rows[i, 0] = i // self.group_rows * 2 + rest // (n * ph)
            rows[i, 1] = rest % ph
        for i in range(self.seg):
            rows[i, 2] = i % n
        for u in range(n):
            for i in range(n * n):
                cols[:2, u * self.lm + i] = u, i // n
        for i in range(self.cols3):
            rest = i % (n * ph)
            cols[2:5, i] = i // self.group_rows, rest // ph, rest % ph
        return [jnp.asarray(rows), jnp.asarray(cols)]


def column_of(row):
    square = (row.shape[1], row.shape[1])
    diagonal = lax.broadcasted_iota(jnp.int32, square, 0) == lax.broadcasted_iota(jnp.int32, square, 1)
    return jnp.sum(jnp.where(diagonal, jnp.broadcast_to(row, square), 0), axis=1, keepdims=True)


def look_up(index, table):
    out = jnp.zeros(index.shape, jnp.int32)
    for k, value in enumerate(table):
        out = out + jnp.where(index == k, value, 0)
    return out


def dot(a, b):
    return jnp.dot(a, b, preferred_element_type=jnp.float32)


def fetch(pairs, sems):
    copies = [pltpu.make_async_copy(src, dst, sems.at[i]) for i, (src, dst) in enumerate(pairs)]
    for copy in copies:
        copy.start()
    return copies


def prep_kernel(
    plan,
    ket, left_h, bond_h, fresh_h, link_h, vert_h, r2_h, c2_h, m2_h, r3_h, c3_h, m3_h, rows_h, cols_h,
    out, k2, k3, gap2, gap3, bond_col,
    wide, left, bond, fresh, link_s, vert_s, r2, c2, m2, r3, c3, m3, rows, cols, sems,
):
    n, half, lm = plan.legs, plan.half, plan.lm
    sources = (link_h, vert_h, bond_h, fresh_h, left_h, r2_h, c2_h, m2_h, r3_h, c3_h, m3_h, rows_h, cols_h)
    targets = (link_s, vert_s, bond, fresh, left, r2, c2, m2, r3, c3, m3, rows, cols)
    copies = fetch(list(zip(sources, targets)), sems)
    for row in range(n * n, lm):
        wide[pl.ds(row, half, stride=lm), :] = jnp.zeros((half, plan.chi), jnp.float32)
    for copy in copies[:5]:
        copy.wait()
    sec = lax.axis_index("sec")
    link = [link_s[0, i] for i in range(n)]
    upper = [vert_s[0, 0, i] for i in range(n)]
    lower = [vert_s[0, 1, i] for i in range(n)]
    fresh_all = column_of(fresh[...])
    fresh_col = jnp.where(sec == 0, fresh_all[:half], fresh_all[half:])
    bond_col[...] = column_of(bond[...])
    gap = fresh_col - bond[...]
    for l in range(n):
        for m in range(n):
            keep = gap == link[l] - link[m]
            val = jnp.where(keep, left[l * n + m].astype(jnp.float32), 0.0)
            wide[pl.ds(l * n + m, half, stride=lm), :] = val
    out[...] = wide[...].astype(jnp.bfloat16)
    for copy in copies[5:]:
        copy.wait()

    def expand(first, second):
        picked = lax.dot_general(first, ket[...], (((1,), (1,)), ((), ())), preferred_element_type=jnp.float32)
        return dot(picked.astype(jnp.bfloat16), second)

    k2[...] = (expand(r2[...], c2[...]) * m2[...].astype(jnp.float32)).astype(jnp.bfloat16)
    total = expand(r3[0], c3[0])
    for p in range(1, plan.phys):
        total = total + expand(r3[p], c3[p])
    k3[...] = (total * m3[...].astype(jnp.float32)).astype(jnp.bfloat16)
    rows_d = look_up(rows[:, 0:1], lower) + rows[:, 1:2]
    gap2[...] = look_up(cols[0:1, :], upper) + look_up(cols[1:2, :], link) - rows_d
    rows_e = look_up(rows[: plan.seg, 2:3], lower)
    c = slice(0, plan.cols3)
    gap3[...] = look_up(cols[2:3, c], upper) + look_up(cols[3:4, c], link) - cols[4:5, c] - rows_e


def halves(first, second):
    sec = lax.axis_index("sec")
    return ((first, sec), (second, 1 - sec))


def pack_lanes(parts, chi):
    lane = lax.broadcasted_iota(jnp.int32, parts[0].shape, 1)
    tiles = []
    for x, part in enumerate(parts):
        first, shift = divmod(x * chi, LANES)
        rolled = pltpu.roll(part, shift, 1) if shift else part
        if first == len(tiles):
            tiles.append(rolled)
        else:
            tiles[first] = jnp.where(lane < shift, tiles[first], rolled)
        if shift + chi > LANES:
            tiles.append(rolled)
    return tiles


def unpack_lanes(tiles, chi, count):
    lane = lax.broadcasted_iota(jnp.int32, tiles[0].shape, 1)
    parts = []
    for x in range(count):
        first, shift = divmod(x * chi, LANES)
        part = tiles[first]
        if shift + chi > LANES:
            part = jnp.where(lane >= shift, part, tiles[first + 1])
        parts.append(pltpu.roll(part, LANES - shift, 1) if shift else part)
    return parts


def first(plan, left, ms, w1, vp):
    chi, lm = plan.chi, plan.lm
    for up in range(plan.pairs):
        both = dot(left, ms[up, vp])
        for k in range(2):
            parts = []
            for x in range(QUAD):
                rows = both[x * lm : (x + 1) * lm]
                parts.append(
                    jnp.concatenate([rows[:, c * LANES : (c + 1) * LANES] for c in (2 * k, 2 * k + 1)], axis=0)
                )
            for t, tile in enumerate(pack_lanes(parts, chi)):
                at = (2 * t + k) * LANES
                w1[vp, up * 2 * lm : (up + 1) * 2 * lm, at : at + LANES] = tile.astype(jnp.bfloat16)


def second(plan, k2, w1, w2, vp, half_of_oct):
    gr, wide = plan.group_rows, QUAD * plan.chi
    out = dot(k2[...], w1[vp])
    for g in range(plan.groups):
        part = out[g * gr : (g + 1) * gr]
        for t in range(wide // LANES):
            pair = [part[:, c * LANES : (c + 1) * LANES] for c in (2 * t, 2 * t + 1)]
            at = half_of_oct * wide + t * LANES
            w2[g, vp * 2 * gr : (vp + 1) * 2 * gr, at : at + LANES] = jnp.concatenate(pair, axis=0).astype(jnp.bfloat16)


def third(plan, k3, w2, w3, g):
    seg = plan.seg
    r, dp = g // plan.pairs, g % plan.pairs
    out = dot(k3[...], w2[g])
    per = QUAD * plan.chi // LANES
    for h in range(2):
        tiles = [out[:, t * LANES : (t + 1) * LANES] for t in range(h * per, (h + 1) * per)]
        for x, part in enumerate(unpack_lanes(tiles, plan.chi, QUAD)):
            part = part.astype(jnp.bfloat16)
            at = (h * QUAD + x) * plan.xrows + dp * seg
            for s in range(plan.legs):
                w3[r, at : at + seg, s * LANES : (s + 1) * LANES] = part[s * seg : (s + 1) * seg]


def fourth(w3, pr, r):
    return lax.dot_general(w3[r], pr[r], (((1,), (1,)), ((), ())), preferred_element_type=jnp.float32)


def add(total, term):
    return term if total is None else total + term


def quad_rows(lhs, plan, quad):
    rows = QUAD * plan.lm
    return lhs[pl.ds(pl.multiple_of(quad * rows, 16), rows), :]


def front_kernel(
    plan,
    link_next_s, bond_next_v, other, lhs, k2_all, k3_all, gap2, gap3, bond_col, mine_h, vert_h,
    ms, k2, k3, w2, w3,
    w1, w2_first, mine, vert_s, sems,
):
    n, chi, half, lanes = plan.legs, plan.chi, plan.half, plan.lanes
    bf16 = jnp.bfloat16
    copies = fetch([(vert_h, vert_s), (mine_h, mine)], sems)
    link_next = [link_next_s[0, i] for i in range(n)]
    tall = plan.pairs * plan.group_rows
    for r in range(n):
        at = slice(r * tall, (r + 1) * tall)
        k2[at] = jnp.where(gap2[...] == link_next[r], k2_all[at].astype(jnp.float32), 0.0).astype(bf16)
        at = slice(r * plan.seg, (r + 1) * plan.seg)
        k3[at] = jnp.where(gap3[...] == link_next[r], k3_all[at].astype(jnp.float32), 0.0).astype(bf16)
    if chi < lanes:
        for k in range(4):
            at = slice(k * lanes + chi, (k + 1) * lanes)
            ms[:, :, :, at] = jnp.zeros((plan.pairs, plan.pairs, chi, lanes - chi), bf16)
    copies[0].wait()
    upper = [vert_s[0, 0, i] for i in range(n)]
    copies[1].wait()
    for src, which in halves(mine, other):
        at = pl.multiple_of(which * half, 16)
        gap = bond_next_v[...] - bond_col[pl.ds(at, half), :]
        for u in range(n):
            for v in range(n):
                keep = gap == upper[u] - upper[v]
                val = jnp.where(keep, src[u * n + v].astype(jnp.float32), 0.0)
                lane = (v % 2 * 2 + u % 2) * lanes
                ms[u // 2, v // 2, pl.ds(at, half), lane : lane + chi] = val.astype(bf16)
    pad = n * plan.lm
    w1[:, :, pad:, :] = jnp.zeros((2, plan.pairs, plan.cols2 - pad, w1.shape[3]), bf16)
    phases = [(o, vp, h) for o in range(2) for vp in range(plan.pairs) for h in range(2)]
    per_g = plan.groups // (2 * plan.pairs)

    def lead(o, vp, h):
        first(plan, quad_rows(lhs, plan, 2 * o + h), ms, w1.at[h], vp)

    lead(*phases[0])
    for i, (o, vp, h) in enumerate(phases):
        if i + 1 < len(phases):
            lead(*phases[i + 1])
        if o:
            at = (2 * vp + h) * per_g
            for g in range(at, at + per_g):
                third(plan, k3, w2_first, w3, g)
        second(plan, k2, w1.at[h], w2 if o else w2_first, vp, h)


def back_kernel(
    plan,
    link_next_s,
    bond_next_v, fresh_next_v, lhs, ms, k2, k3, w2_in, w3_in, pr_mine, pr_other,
    image, partial, w2_odd, w3_even,
    pr, w1, w2_even, w3_odd,
):
    n, chi, half, lanes = plan.legs, plan.chi, plan.half, plan.lanes
    bf16 = jnp.bfloat16
    link_next = [link_next_s[0, i] for i in range(n)]
    fresh_col = column_of(fresh_next_v[...])
    pr[...] = jnp.zeros_like(pr)
    for src, which in halves(pr_mine, pr_other):
        at = pl.multiple_of(which * half, 16)
        gap = jnp.where(which == 0, fresh_col[:half], fresh_col[half:]) - bond_next_v[...]
        for r in range(n):
            for s in range(n):
                keep = gap == link_next[r] - link_next[s]
                val = jnp.where(keep, src[r * n + s].astype(jnp.float32), 0.0)
                pr[r, pl.ds(at, half), s * lanes : s * lanes + chi] = val.astype(bf16)
    pad = n * plan.lm
    w1[:, :, pad:, :] = jnp.zeros((2, plan.pairs, plan.cols2 - pad, w1.shape[3]), bf16)

    del w2_in, w3_in
    block = 2 * QUAD * plan.xrows
    per_g = plan.groups // (2 * plan.pairs)
    per_r = n // (2 * plan.pairs)
    w2, w3 = (w2_even, w2_odd), (w3_even, w3_odd)

    def put(oct, total):
        image[pl.ds(pl.multiple_of(oct * block, 8), block), :] = total
        return jnp.sum(total * total)

    def body(j, square_sum):
        def lead(k, vp, h):
            first(plan, quad_rows(lhs, plan, 2 * (2 * j + k + 2) + h), ms, w1.at[h], vp)

        phases = [(k, vp, h) for k in range(2) for vp in range(plan.pairs) for h in range(2)]
        total = None
        lead(*phases[0])
        for i, (k, vp, h) in enumerate(phases):
            if i + 1 < len(phases):
                lead(*phases[i + 1])
            phase = 2 * vp + h
            for g in range(phase * per_g, (phase + 1) * per_g):
                third(plan, k3, w2[1 - k], w3[1 - k], g)
            for r in range(phase * per_r, (phase + 1) * per_r):
                total = add(total, fourth(w3[k], pr, r))
            second(plan, k2, w1.at[h], w2[k], vp, h)
            if phase == 2 * plan.pairs - 1:
                square_sum = square_sum + put(2 * j + k, total)
                total = None
        return square_sum

    octs = half // (2 * QUAD)
    square_sum = lax.fori_loop(0, (octs - 2) // 2, body, jnp.float32(0.0))
    total = None
    for g in range(plan.groups):
        third(plan, k3, w2_odd, w3_odd, g)
        if g % plan.pairs == 0:
            total = add(total, fourth(w3_even, pr, g // plan.pairs))
    square_sum = square_sum + put(octs - 2, total)
    even = odd = None
    for r in range(0, n, 2):
        even = add(even, fourth(w3_odd, pr, r))
        odd = add(odd, fourth(w3_odd, pr, r + 1))
    square_sum = square_sum + put(octs - 1, even + odd)
    partial[...] = jnp.full_like(partial, square_sum)


def finish_kernel(plan, count, columns, incoming, image, new, log_norm):
    n, half = plan.legs, plan.half
    sums = incoming[...]
    devices = sums.shape[0]
    row = lax.broadcasted_iota(jnp.int32, sums.shape, 0)
    pair = sums + pltpu.roll(sums, devices - 1, 0)
    logs = 0.5 * jnp.log(pair / count + 1e-06)
    log_norm[0, 0] = jnp.sum(jnp.where(row % 2 == 0, logs, 0.0)[:, :1]) / columns
    here = jnp.sum(jnp.where(row == 2 * lax.axis_index("col"), pair, 0.0), axis=0, keepdims=True)
    scale = lax.rsqrt(here / count + 1e-06)[:, : plan.chi]
    for d in range(n):
        for e in range(n):
            at = (d // 2) * plan.seg + (d % 2) * n + e
            new[d * n + e] = (image[pl.ds(at, half, stride=plan.xrows), :] * scale).astype(jnp.bfloat16)


def whole(memory, count):
    return [pl.BlockSpec(memory_space=memory) for _ in range(count)]


def absorb_row(mps, ket, left_proj, right_proj, bond_charge, new_charge, link_charge, vert_charge):
    half, chi, legs = left_proj.shape[1], left_proj.shape[2], left_proj.shape[3]
    phys = ket.shape[5]
    plan = Plan(chi, half, legs, phys)
    squared = legs * legs
    columns, sections = lax.axis_size("col"), lax.axis_size("sec")
    bf16, f32 = jnp.bfloat16, jnp.float32
    smem, vmem = pltpu.SMEM, pltpu.VMEM
    swap = [(i, 1 - i) for i in range(sections)]
    hbm = pltpu.HBM
    bond_next, fresh_next, link_next = from_behind((bond_charge, new_charge, link_charge), "col", -1)
    mine = jnp.transpose(mps[0], (1, 2, 0, 3)).reshape(squared, half, chi)
    other = lax.ppermute(mine, "sec", swap)
    pr_mine = from_behind(jnp.transpose(right_proj[0], (1, 2, 3, 0)).reshape(squared, half, chi), "col", -1)
    bond_next, fresh_next, link_next = lax.optimization_barrier((bond_next, fresh_next, link_next))
    left = jnp.transpose(left_proj[0], (2, 3, 0, 1)).reshape(squared, half, chi)
    flat_ket = jnp.transpose(ket[0], (0, 1, 2, 4, 3)).reshape(squared, squared * phys)
    fetched = [left, bond_charge, new_charge, link_charge, vert_charge] + plan.matrices() + plan.indices()
    in_smem = (3, 4)
    scratch = [(smem if i in in_smem else vmem)(x.shape, x.dtype) for i, x in enumerate(fetched)]
    scratch = [scratch[i] for i in (0, 1, 2, 3, 4)] + scratch[5:]
    lhs, *kets = pl.pallas_call(
        functools.partial(prep_kernel, plan),
        in_specs=whole(vmem, 1) + whole(hbm, len(fetched)),
        out_specs=whole(vmem, 6),
        out_shape=[
            jax.ShapeDtypeStruct((half * plan.lm, chi), bf16),
            jax.ShapeDtypeStruct((plan.rows2, plan.cols2), bf16),
            jax.ShapeDtypeStruct((plan.rows3, plan.cols3), bf16),
            jax.ShapeDtypeStruct((squared * phys, plan.cols2), jnp.int32),
            jax.ShapeDtypeStruct((plan.seg, plan.cols3), jnp.int32),
            jax.ShapeDtypeStruct((chi, 1), jnp.int32),
        ],
        scratch_shapes=[pltpu.VMEM((half * plan.lm, chi), f32)] + scratch + [pltpu.SemaphoreType.DMA((len(fetched),))],
        compiler_params=pltpu.CompilerParams(vmem_limit_bytes=12 << 20),
        cost_estimate=pl.CostEstimate(flops=FRONT_FLOPS // 8, bytes_accessed=1 << 20, transcendentals=0),
        name="prep",
    )(flat_ket, *[pltpu.with_memory_space_constraint(x, pltpu.HBM) for x in fetched])
    octs = half // (2 * QUAD)
    if half % (2 * QUAD) or octs % 2 or (QUAD * chi) % LANES:
        raise ValueError("half")
    block = 2 * QUAD * plan.xrows
    lanes = plan.lanes
    wide = 2 * QUAD * chi
    w1_shape = (2, plan.pairs, plan.cols2, wide)
    w2_shape = jax.ShapeDtypeStruct((plan.groups, plan.cols3, wide), bf16)
    w3_shape = jax.ShapeDtypeStruct((legs, block, legs * lanes), bf16)
    operands = [link_next, bond_next, other, lhs] + kets
    operands += [pltpu.with_memory_space_constraint(x, pltpu.HBM) for x in (mine, vert_charge)]
    ms, k2, k3, w2, w3 = pl.pallas_call(
        functools.partial(front_kernel, plan),
        in_specs=whole(smem, 1) + whole(vmem, len(operands) - 3) + whole(hbm, 2),
        out_specs=whole(vmem, 5),
        out_shape=[
            jax.ShapeDtypeStruct((plan.pairs, plan.pairs, chi, 4 * lanes), bf16),
            jax.ShapeDtypeStruct((plan.rows2, plan.cols2), bf16),
            jax.ShapeDtypeStruct((plan.rows3, plan.cols3), bf16),
            w2_shape,
            w3_shape,
        ],
        scratch_shapes=[
            pltpu.VMEM(w1_shape, bf16),
            pltpu.VMEM(w2_shape.shape, bf16),
            pltpu.VMEM(mine.shape, bf16),
            pltpu.SMEM(vert_charge.shape, jnp.int32),
            pltpu.SemaphoreType.DMA((2,)),
        ],
        compiler_params=pltpu.CompilerParams(vmem_limit_bytes=VMEM_LIMIT),
        cost_estimate=pl.CostEstimate(flops=FRONT_FLOPS, bytes_accessed=1 << 20, transcendentals=0),
        name="front",
    )(*operands)
    pr_mine, w3 = lax.optimization_barrier((pr_mine, w3))
    pr_other = lax.ppermute(pr_mine, "sec", swap)
    operands = [link_next, bond_next, fresh_next, lhs, ms, k2, k3, w2, w3, pr_mine, pr_other]
    image, partial, _, _ = pl.pallas_call(
        functools.partial(back_kernel, plan),
        in_specs=whole(smem, 1) + whole(vmem, len(operands) - 1),
        out_specs=whole(vmem, 4),
        out_shape=[
            jax.ShapeDtypeStruct((octs * block, chi), f32),
            jax.ShapeDtypeStruct((columns * sections, 1, LANES), f32),
            w2_shape,
            w3_shape,
        ],
        input_output_aliases={7: 2, 8: 3},
        scratch_shapes=[
            pltpu.VMEM((legs, chi, legs * lanes), bf16),
            pltpu.VMEM(w1_shape, bf16),
            pltpu.VMEM(w2_shape.shape, bf16),
            pltpu.VMEM(w3_shape.shape, bf16),
        ],
        compiler_params=pltpu.CompilerParams(vmem_limit_bytes=VMEM_LIMIT),
        cost_estimate=pl.CostEstimate(flops=2 * FRONT_FLOPS, bytes_accessed=1 << 20, transcendentals=0),
        name="back",
    )(*operands)
    incoming = lax.all_to_all(partial, ("col", "sec"), 0, 0, tiled=True)
    new, log_norm = pl.pallas_call(
        functools.partial(finish_kernel, plan, float(chi * squared * chi), float(columns)),
        in_specs=whole(vmem, 2),
        out_specs=whole(vmem, 1) + whole(smem, 1),
        out_shape=[
            jax.ShapeDtypeStruct((squared, half, chi), bf16),
            jax.ShapeDtypeStruct((1, 1), f32),
        ],
        compiler_params=pltpu.CompilerParams(vmem_limit_bytes=8 << 20),
        name="finish",
    )(incoming.reshape(columns * sections, LANES), image)
    new_mps = jnp.transpose(new.reshape(legs, legs, half, chi), (2, 0, 1, 3))[None]
    return (new_mps, log_norm.reshape(()))


def solution(mesh):
    placed = (
        P("col", "sec", None, None, None),
        P("col", None, None, None, None, None),
        P("col", "sec", None, None, None),
        P("col", None, None, None, "sec"),
        P("col", None),
        P("col", None),
        P("col", None),
        P("col", None, None),
    )
    return jax.shard_map(
        absorb_row,
        mesh=mesh,
        in_specs=placed,
        out_specs=(P("col", "sec", None, None, None), P()),
        check_vma=False,
    )
```

```python
import functools

import jax
import jax.numpy as jnp
import numpy as np
from jax import lax
from jax.experimental import pallas as pl
from jax.experimental.pallas import tpu as pltpu
from jax.sharding import PartitionSpec as P

LANES = 128
QUAD = 4
VMEM_LIMIT = 36 << 20
FRONT_FLOPS = 1 << 30


def round_up(value, multiple):
    return -(-value // multiple) * multiple


def from_behind(x, axis, by):
    count = lax.axis_size(axis)
    return lax.ppermute(x, axis, [(i, (i + by) % count) for i in range(count)])


class Plan:
    def __init__(self, chi, half, legs, phys):
        self.chi, self.half, self.legs, self.phys = chi, half, legs, phys
        self.lanes = round_up(chi, LANES)
        self.lm = round_up(legs * legs, 8)
        self.pairs = legs // 2
        self.group_rows = 2 * legs * phys
        self.groups = legs * self.pairs
        self.rows2 = self.groups * self.group_rows
        self.cols2 = round_up(legs * self.lm, 256)
        self.seg = round_up(2 * legs, 16)
        self.rows3 = legs * self.seg
        self.cols3 = legs * self.group_rows
        self.xrows = self.pairs * self.seg

    def matrices(self):
        n, ph = self.legs, self.phys
        wide = n * n * ph
        r2 = np.zeros((self.rows2, wide), np.float32)
        row_m = np.zeros((self.rows2,), np.int64)
        for r in range(n):
            for d in range(n):
                for m in range(n):
                    for p in range(ph):
                        g = r * self.pairs + d // 2
                        row = g * self.group_rows + (d % 2) * n * ph + m * ph + p
                        r2[row, (d * ph + p) * n + r] = 1
                        row_m[row] = m
        c2 = np.zeros((n * n, self.cols2), np.float32)
        col_m = np.full((self.cols2,), -1)
        for u in range(n):
            for l in range(n):
                for m in range(n):
                    c = u * self.lm + l * n + m
                    c2[u * n + l, c] = 1
                    col_m[c] = m
        m2 = row_m[:, None] == col_m[None, :]
        r3 = np.zeros((ph, self.rows3, wide), np.float32)
        row_d = np.full((self.rows3,), -1)
        for s in range(n):
            for d2 in range(2):
                for e in range(n):
                    row = s * self.seg + d2 * n + e
                    row_d[row] = d2
                    for p in range(ph):
                        r3[p, row, (e * ph + p) * n + s] = 1
        c3 = np.zeros((ph, n * n, self.cols3), np.float32)
        col_d = np.zeros((self.cols3,), np.int64)
        for v in range(n):
            for d2 in range(2):
                for m in range(n):
                    for p in range(ph):
                        col = v * self.group_rows + d2 * n * ph + m * ph + p
                        c3[p, v * n + m, col] = 1
                        col_d[col] = d2
        m3 = row_d[:, None] == col_d[None, :]
        return [jnp.asarray(x, jnp.bfloat16) for x in (r2, c2, m2, r3, c3, m3)]

    def indices(self):
        n, ph = self.legs, self.phys
        rows = np.zeros((n * n * ph, 8), np.int32)
        cols = np.zeros((8, self.cols2), np.int32)
        for i in range(n * n * ph):
            rest = i % self.group_rows
            rows[i, 0] = i // self.group_rows * 2 + rest // (n * ph)
            rows[i, 1] = rest % ph
        for i in range(self.seg):
            rows[i, 2] = i % n
        for u in range(n):
            for i in range(n * n):
                cols[:2, u * self.lm + i] = u, i // n
        for i in range(self.cols3):
            rest = i % (n * ph)
            cols[2:5, i] = i // self.group_rows, rest // ph, rest % ph
        return [jnp.asarray(rows), jnp.asarray(cols)]


def column_of(row):
    square = (row.shape[1], row.shape[1])
    diagonal = lax.broadcasted_iota(jnp.int32, square, 0) == lax.broadcasted_iota(jnp.int32, square, 1)
    return jnp.sum(jnp.where(diagonal, jnp.broadcast_to(row, square), 0), axis=1, keepdims=True)


def look_up(index, table):
    out = jnp.zeros(index.shape, jnp.int32)
    for k, value in enumerate(table):
        out = out + jnp.where(index == k, value, 0)
    return out


def dot(a, b):
    return jnp.dot(a, b, preferred_element_type=jnp.float32)


def fetch(pairs, sems):
    copies = [pltpu.make_async_copy(src, dst, sems.at[i]) for i, (src, dst) in enumerate(pairs)]
    for copy in copies:
        copy.start()
    return copies


def prep_kernel(
    plan,
    ket, left_h, bond_h, fresh_h, link_h, vert_h, r2_h, c2_h, m2_h, r3_h, c3_h, m3_h, rows_h, cols_h,
    out, k2, k3, gap2, gap3, bond_col,
    wide, left, bond, fresh, link_s, vert_s, r2, c2, m2, r3, c3, m3, rows, cols, sems,
):
    n, half, lm = plan.legs, plan.half, plan.lm
    sources = (link_h, vert_h, bond_h, fresh_h, left_h, r2_h, c2_h, m2_h, r3_h, c3_h, m3_h, rows_h, cols_h)
    targets = (link_s, vert_s, bond, fresh, left, r2, c2, m2, r3, c3, m3, rows, cols)
    copies = fetch(list(zip(sources, targets)), sems)
    for row in range(n * n, lm):
        wide[pl.ds(row, half, stride=lm), :] = jnp.zeros((half, plan.chi), jnp.float32)
    for copy in copies[:5]:
        copy.wait()
    sec = lax.axis_index("sec")
    link = [link_s[0, i] for i in range(n)]
    upper = [vert_s[0, 0, i] for i in range(n)]
    lower = [vert_s[0, 1, i] for i in range(n)]
    fresh_all = column_of(fresh[...])
    fresh_col = jnp.where(sec == 0, fresh_all[:half], fresh_all[half:])
    bond_col[...] = column_of(bond[...])
    gap = fresh_col - bond[...]
    for l in range(n):
        for m in range(n):
            keep = gap == link[l] - link[m]
            val = jnp.where(keep, left[l * n + m].astype(jnp.float32), 0.0)
            wide[pl.ds(l * n + m, half, stride=lm), :] = val
    out[...] = wide[...].astype(jnp.bfloat16)
    for copy in copies[5:]:
        copy.wait()

    def expand(first, second):
        picked = lax.dot_general(first, ket[...], (((1,), (1,)), ((), ())), preferred_element_type=jnp.float32)
        return dot(picked.astype(jnp.bfloat16), second)

    k2[...] = (expand(r2[...], c2[...]) * m2[...].astype(jnp.float32)).astype(jnp.bfloat16)
    total = expand(r3[0], c3[0])
    for p in range(1, plan.phys):
        total = total + expand(r3[p], c3[p])
    k3[...] = (total * m3[...].astype(jnp.float32)).astype(jnp.bfloat16)
    rows_d = look_up(rows[:, 0:1], lower) + rows[:, 1:2]
    gap2[...] = look_up(cols[0:1, :], upper) + look_up(cols[1:2, :], link) - rows_d
    rows_e = look_up(rows[: plan.seg, 2:3], lower)
    c = slice(0, plan.cols3)
    gap3[...] = look_up(cols[2:3, c], upper) + look_up(cols[3:4, c], link) - cols[4:5, c] - rows_e


def halves(first, second):
    sec = lax.axis_index("sec")
    return ((first, sec), (second, 1 - sec))


def pack_lanes(parts, chi):
    lane = lax.broadcasted_iota(jnp.int32, parts[0].shape, 1)
    tiles = []
    for x, part in enumerate(parts):
        first, shift = divmod(x * chi, LANES)
        rolled = pltpu.roll(part, shift, 1) if shift else part
        if first == len(tiles):
            tiles.append(rolled)
        else:
            tiles[first] = jnp.where(lane < shift, tiles[first], rolled)
        if shift + chi > LANES:
            tiles.append(rolled)
    return tiles


def unpack_lanes(tiles, chi, count):
    lane = lax.broadcasted_iota(jnp.int32, tiles[0].shape, 1)
    parts = []
    for x in range(count):
        first, shift = divmod(x * chi, LANES)
        part = tiles[first]
        if shift + chi > LANES:
            part = jnp.where(lane >= shift, part, tiles[first + 1])
        parts.append(pltpu.roll(part, LANES - shift, 1) if shift else part)
    return parts


def first(plan, left, ms, w1, vp):
    chi, lm = plan.chi, plan.lm
    for up in range(plan.pairs):
        both = dot(left, ms[up, vp])
        for k in range(2):
            parts = []
            for x in range(QUAD):
                rows = both[x * lm : (x + 1) * lm]
                parts.append(
                    jnp.concatenate([rows[:, c * LANES : (c + 1) * LANES] for c in (2 * k, 2 * k + 1)], axis=0)
                )
            for t, tile in enumerate(pack_lanes(parts, chi)):
                at = (2 * t + k) * LANES
                w1[vp, up * 2 * lm : (up + 1) * 2 * lm, at : at + LANES] = tile.astype(jnp.bfloat16)


def second(plan, k2, w1, w2, vp, half_of_oct):
    gr, wide = plan.group_rows, QUAD * plan.chi
    out = dot(k2[...], w1[vp])
    for g in range(plan.groups):
        part = out[g * gr : (g + 1) * gr]
        for t in range(wide // LANES):
            pair = [part[:, c * LANES : (c + 1) * LANES] for c in (2 * t, 2 * t + 1)]
            at = half_of_oct * wide + t * LANES
            w2[g, vp * 2 * gr : (vp + 1) * 2 * gr, at : at + LANES] = jnp.concatenate(pair, axis=0).astype(jnp.bfloat16)


def third(plan, k3, w2, w3, g):
    seg = plan.seg
    r, dp = g // plan.pairs, g % plan.pairs
    out = dot(k3[...], w2[g])
    per = QUAD * plan.chi // LANES
    for h in range(2):
        tiles = [out[:, t * LANES : (t + 1) * LANES] for t in range(h * per, (h + 1) * per)]
        for x, part in enumerate(unpack_lanes(tiles, plan.chi, QUAD)):
            part = part.astype(jnp.bfloat16)
            at = (h * QUAD + x) * plan.xrows + dp * seg
            for s in range(plan.legs):
                w3[r, at : at + seg, s * LANES : (s + 1) * LANES] = part[s * seg : (s + 1) * seg]


def fourth(w3, pr, r):
    return lax.dot_general(w3[r], pr[r], (((1,), (1,)), ((), ())), preferred_element_type=jnp.float32)


def add(total, term):
    return term if total is None else total + term


def quad_rows(lhs, plan, quad):
    rows = QUAD * plan.lm
    return lhs[pl.ds(pl.multiple_of(quad * rows, 16), rows), :]


def front_kernel(
    plan,
    charges_s, charges_v, other, lhs, k2_all, k3_all, gap2, gap3, bond_col, mine_h, vert_h,
    ms, k2, k3, w2, w3_a, w3_b,
    w1, w2_a, w2_b, mine, vert_s, sems,
):
    n, chi, half, lanes = plan.legs, plan.chi, plan.half, plan.lanes
    bf16 = jnp.bfloat16
    copies = fetch([(vert_h, vert_s), (mine_h, mine)], sems)
    link_next = [charges_s[2, i] for i in range(n)]
    bond_next = charges_v[0:1, :]
    tall = plan.pairs * plan.group_rows
    for r in range(n):
        at = slice(r * tall, (r + 1) * tall)
        k2[at] = jnp.where(gap2[...] == link_next[r], k2_all[at].astype(jnp.float32), 0.0).astype(bf16)
        at = slice(r * plan.seg, (r + 1) * plan.seg)
        k3[at] = jnp.where(gap3[...] == link_next[r], k3_all[at].astype(jnp.float32), 0.0).astype(bf16)
    if chi < lanes:
        for k in range(4):
            at = slice(k * lanes + chi, (k + 1) * lanes)
            ms[:, :, :, at] = jnp.zeros((plan.pairs, plan.pairs, chi, lanes - chi), bf16)
    copies[0].wait()
    upper = [vert_s[0, 0, i] for i in range(n)]
    copies[1].wait()
    for src, which in halves(mine, other):
        at = pl.multiple_of(which * half, 16)
        gap = bond_next - bond_col[pl.ds(at, half), :]
        for u in range(n):
            for v in range(n):
                keep = gap == upper[u] - upper[v]
                val = jnp.where(keep, src[u * n + v].astype(jnp.float32), 0.0)
                lane = (v % 2 * 2 + u % 2) * lanes
                ms[u // 2, v // 2, pl.ds(at, half), lane : lane + chi] = val.astype(bf16)
    pad = n * plan.lm
    w1[:, :, pad:, :] = jnp.zeros((2, plan.pairs, plan.cols2 - pad, w1.shape[3]), bf16)
    phases = [(o, vp, h) for o in range(3) for vp in range(plan.pairs) for h in range(2)]
    per_g = plan.groups // (2 * plan.pairs)
    chain, done = (w2_a, w2_b, w2), (w3_a, w3_b)

    def lead(o, vp, h):
        first(plan, quad_rows(lhs, plan, 2 * o + h), ms, w1.at[h], vp)

    lead(*phases[0])
    for i, (o, vp, h) in enumerate(phases):
        if i + 1 < len(phases):
            lead(*phases[i + 1])
        if o:
            at = (2 * vp + h) * per_g
            for g in range(at, at + per_g):
                third(plan, k3, chain[o - 1], done[o - 1], g)
        second(plan, k2, w1.at[h], chain[o], vp, h)


def middle_kernel(plan, lhs, ms, k2, k3, w2_in, w2, w3, w1):
    pad = plan.legs * plan.lm
    w1[:, :, pad:, :] = jnp.zeros((2, plan.pairs, plan.cols2 - pad, w1.shape[3]), jnp.bfloat16)
    phases = [(vp, h) for vp in range(plan.pairs) for h in range(2)]
    per_g = plan.groups // len(phases)

    def lead(vp, h):
        first(plan, quad_rows(lhs, plan, 6 + h), ms, w1.at[h], vp)

    lead(*phases[0])
    for i, (vp, h) in enumerate(phases):
        if i + 1 < len(phases):
            lead(*phases[i + 1])
        for g in range(i * per_g, (i + 1) * per_g):
            third(plan, k3, w2_in, w3, g)
        second(plan, k2, w1.at[h], w2, vp, h)


def back_kernel(
    plan,
    charges_s,
    charges_v, lhs, ms, k2, k3, w2_in, w3_a, w3_b, w3_c, pr_mine, pr_other,
    image, partial,
    pr, w1, w2_a, w2_b, w3_d, w3_e, w3_f,
):
    n, chi, half, lanes = plan.legs, plan.chi, plan.half, plan.lanes
    bf16 = jnp.bfloat16
    link_next = [charges_s[2, i] for i in range(n)]
    bond_next = charges_v[0:1, :]
    fresh_col = column_of(charges_v[1:2, :])
    pr[...] = jnp.zeros_like(pr)
    for src, which in halves(pr_mine, pr_other):
        at = pl.multiple_of(which * half, 16)
        gap = jnp.where(which == 0, fresh_col[:half], fresh_col[half:]) - bond_next
        for r in range(n):
            for s in range(n):
                keep = gap == link_next[r] - link_next[s]
                val = jnp.where(keep, src[r * n + s].astype(jnp.float32), 0.0)
                pr[r, pl.ds(at, half), s * lanes : s * lanes + chi] = val.astype(bf16)
    pad = n * plan.lm
    w1[:, :, pad:, :] = jnp.zeros((2, plan.pairs, plan.cols2 - pad, w1.shape[3]), bf16)

    block = 2 * QUAD * plan.xrows
    per_g = plan.groups // (2 * plan.pairs)
    per_r = n // (2 * plan.pairs)

    def put(oct, total):
        image[oct * block : (oct + 1) * block, :] = total
        return jnp.sum(total * total)

    w2 = (w2_in, w2_a, w2_b)
    w3 = (w3_a, w3_b, w3_c, w3_d, w3_e, w3_f)
    phases = [(o, vp, h) for o in range(2) for vp in range(plan.pairs) for h in range(2)]

    def lead(o, vp, h):
        first(plan, quad_rows(lhs, plan, 2 * (o + 4) + h), ms, w1.at[h], vp)

    square_sum = 0.0
    total = None
    lead(*phases[0])
    for i, (o, vp, h) in enumerate(phases):
        if i + 1 < len(phases):
            lead(*phases[i + 1])
        phase = 2 * vp + h
        for g in range(phase * per_g, (phase + 1) * per_g):
            third(plan, k3, w2[o], w3[o + 3], g)
        for r in range(phase * per_r, (phase + 1) * per_r):
            total = add(total, fourth(w3[o], pr, r))
        second(plan, k2, w1.at[h], w2[o + 1], vp, h)
        if phase == 2 * plan.pairs - 1:
            square_sum = square_sum + put(o, total)
            total = None
    partial[...] = jnp.full_like(partial, square_sum)

    @pl.when(lax.axis_index("sec") >= 0)
    def _():
        square_sum = 0.0
        total = None
        for g in range(plan.groups):
            third(plan, k3, w2[2], w3[5], g)
            if g % plan.pairs == 0:
                total = add(total, fourth(w3[2], pr, g // plan.pairs))
        square_sum = square_sum + put(2, total)
        for o in range(3, 6):
            even = odd = None
            for r in range(0, n, 2):
                even = add(even, fourth(w3[o], pr, r))
                odd = add(odd, fourth(w3[o], pr, r + 1))
            square_sum = square_sum + put(o, even + odd)
        partial[...] += jnp.full_like(partial, square_sum)


def finish_kernel(plan, count, columns, incoming, image, new, log_norm):
    n, half = plan.legs, plan.half
    sums = incoming[...]
    devices = sums.shape[0]
    row = lax.broadcasted_iota(jnp.int32, sums.shape, 0)
    pair = sums + pltpu.roll(sums, devices - 1, 0)
    logs = 0.5 * jnp.log(pair / count + 1e-06)
    log_norm[0, 0] = jnp.sum(jnp.where(row % 2 == 0, logs, 0.0)[:, :1]) / columns
    here = jnp.sum(jnp.where(row == 2 * lax.axis_index("col"), pair, 0.0), axis=0, keepdims=True)
    scale = lax.rsqrt(here / count + 1e-06)[:, : plan.chi]
    for d in range(n):
        for e in range(n):
            at = (d // 2) * plan.seg + (d % 2) * n + e
            new[d * n + e] = (image[pl.ds(at, half, stride=plan.xrows), :] * scale).astype(jnp.bfloat16)


def whole(memory, count):
    return [pl.BlockSpec(memory_space=memory) for _ in range(count)]


def absorb_row(mps, ket, left_proj, right_proj, bond_charge, new_charge, link_charge, vert_charge):
    half, chi, legs = left_proj.shape[1], left_proj.shape[2], left_proj.shape[3]
    phys = ket.shape[5]
    plan = Plan(chi, half, legs, phys)
    squared = legs * legs
    columns, sections = lax.axis_size("col"), lax.axis_size("sec")
    bf16, f32 = jnp.bfloat16, jnp.float32
    smem, vmem = pltpu.SMEM, pltpu.VMEM
    swap = [(i, 1 - i) for i in range(sections)]
    hbm = pltpu.HBM
    link_row = jnp.pad(link_charge, ((0, 0), (0, chi - legs)))
    charges = from_behind(jnp.concatenate([bond_charge, new_charge, link_row], axis=0), "col", -1)
    mine = jnp.transpose(mps[0], (1, 2, 0, 3)).reshape(squared, half, chi)
    other = lax.ppermute(mine, "sec", swap)
    pr_mine = from_behind(jnp.transpose(right_proj[0], (1, 2, 3, 0)).reshape(squared, half, chi), "col", -1)
    left = jnp.transpose(left_proj[0], (2, 3, 0, 1)).reshape(squared, half, chi)
    flat_ket = jnp.transpose(ket[0], (0, 1, 2, 4, 3)).reshape(squared, squared * phys)
    fetched = [left, bond_charge, new_charge, link_charge, vert_charge] + plan.matrices() + plan.indices()
    in_smem = (3, 4)
    scratch = [(smem if i in in_smem else vmem)(x.shape, x.dtype) for i, x in enumerate(fetched)]
    scratch = [scratch[i] for i in (0, 1, 2, 3, 4)] + scratch[5:]
    lhs, *kets = pl.pallas_call(
        functools.partial(prep_kernel, plan),
        in_specs=whole(vmem, 1) + whole(hbm, len(fetched)),
        out_specs=whole(vmem, 6),
        out_shape=[
            jax.ShapeDtypeStruct((half * plan.lm, chi), bf16),
            jax.ShapeDtypeStruct((plan.rows2, plan.cols2), bf16),
            jax.ShapeDtypeStruct((plan.rows3, plan.cols3), bf16),
            jax.ShapeDtypeStruct((squared * phys, plan.cols2), jnp.int32),
            jax.ShapeDtypeStruct((plan.seg, plan.cols3), jnp.int32),
            jax.ShapeDtypeStruct((chi, 1), jnp.int32),
        ],
        scratch_shapes=[pltpu.VMEM((half * plan.lm, chi), f32)] + scratch + [pltpu.SemaphoreType.DMA((len(fetched),))],
        compiler_params=pltpu.CompilerParams(vmem_limit_bytes=12 << 20),
        cost_estimate=pl.CostEstimate(flops=FRONT_FLOPS // 8, bytes_accessed=1 << 20, transcendentals=0),
        name="prep",
    )(flat_ket, *[pltpu.with_memory_space_constraint(x, pltpu.HBM) for x in fetched])
    octs = half // (2 * QUAD)
    if half % (2 * QUAD) or octs != 6 or (QUAD * chi) % LANES:
        raise ValueError("half")
    block = 2 * QUAD * plan.xrows
    lanes = plan.lanes
    wide = 2 * QUAD * chi
    w1_shape = (2, plan.pairs, plan.cols2, wide)
    w2_shape = jax.ShapeDtypeStruct((plan.groups, plan.cols3, wide), bf16)
    w3_shape = jax.ShapeDtypeStruct((legs, block, legs * lanes), bf16)
    operands = [charges, charges, other, lhs] + kets
    operands += [pltpu.with_memory_space_constraint(x, pltpu.HBM) for x in (mine, vert_charge)]
    ms, k2, k3, w2, *w3 = pl.pallas_call(
        functools.partial(front_kernel, plan),
        in_specs=whole(smem, 1) + whole(vmem, len(operands) - 3) + whole(hbm, 2),
        out_specs=whole(vmem, 6),
        out_shape=[
            jax.ShapeDtypeStruct((plan.pairs, plan.pairs, chi, 4 * lanes), bf16),
            jax.ShapeDtypeStruct((plan.rows2, plan.cols2), bf16),
            jax.ShapeDtypeStruct((plan.rows3, plan.cols3), bf16),
            w2_shape,
            w3_shape,
            w3_shape,
        ],
        scratch_shapes=[
            pltpu.VMEM(w1_shape, bf16),
            pltpu.VMEM(w2_shape.shape, bf16),
            pltpu.VMEM(w2_shape.shape, bf16),
            pltpu.VMEM(mine.shape, bf16),
            pltpu.SMEM(vert_charge.shape, jnp.int32),
            pltpu.SemaphoreType.DMA((2,)),
        ],
        compiler_params=pltpu.CompilerParams(vmem_limit_bytes=VMEM_LIMIT),
        cost_estimate=pl.CostEstimate(flops=FRONT_FLOPS, bytes_accessed=1 << 20, transcendentals=0),
        name="front",
    )(*operands)
    pr_mine, w2 = lax.optimization_barrier((pr_mine, w2))
    pr_other = lax.ppermute(pr_mine, "sec", swap)
    w2, w3_last = pl.pallas_call(
        functools.partial(middle_kernel, plan),
        in_specs=whole(vmem, 5),
        out_specs=whole(vmem, 2),
        out_shape=[w2_shape, w3_shape],
        scratch_shapes=[pltpu.VMEM(w1_shape, bf16)],
        compiler_params=pltpu.CompilerParams(vmem_limit_bytes=20 << 20),
        cost_estimate=pl.CostEstimate(flops=FRONT_FLOPS, bytes_accessed=1 << 20, transcendentals=0),
        name="middle",
    )(lhs, ms, k2, k3, w2)
    operands = [charges, charges, lhs, ms, k2, k3, w2, *w3, w3_last, pr_mine, pr_other]
    image, partial = pl.pallas_call(
        functools.partial(back_kernel, plan),
        in_specs=whole(smem, 1) + whole(vmem, len(operands) - 1),
        out_specs=whole(vmem, 2),
        out_shape=[
            jax.ShapeDtypeStruct((octs * block, chi), f32),
            jax.ShapeDtypeStruct((columns * sections, 1, LANES), f32),
        ],
        scratch_shapes=[
            pltpu.VMEM((legs, chi, legs * lanes), bf16),
            pltpu.VMEM(w1_shape, bf16),
        ]
        + [pltpu.VMEM(w2_shape.shape, bf16)] * 2
        + [pltpu.VMEM(w3_shape.shape, bf16)] * 3,
        compiler_params=pltpu.CompilerParams(vmem_limit_bytes=VMEM_LIMIT),
        cost_estimate=pl.CostEstimate(flops=2 * FRONT_FLOPS, bytes_accessed=1 << 20, transcendentals=0),
        name="back",
    )(*operands)
    incoming = lax.all_to_all(partial, ("col", "sec"), 0, 0, tiled=True)
    new, log_norm = pl.pallas_call(
        functools.partial(finish_kernel, plan, float(chi * squared * chi), float(columns)),
        in_specs=whole(vmem, 2),
        out_specs=whole(vmem, 1) + whole(smem, 1),
        out_shape=[
            jax.ShapeDtypeStruct((squared, half, chi), bf16),
            jax.ShapeDtypeStruct((1, 1), f32),
        ],
        compiler_params=pltpu.CompilerParams(vmem_limit_bytes=8 << 20),
        name="finish",
    )(incoming.reshape(columns * sections, LANES), image)
    new_mps = jnp.transpose(new.reshape(legs, legs, half, chi), (2, 0, 1, 3))[None]
    return (new_mps, log_norm.reshape(()))


def solution(mesh):
    placed = (
        P("col", "sec", None, None, None),
        P("col", None, None, None, None, None),
        P("col", "sec", None, None, None),
        P("col", None, None, None, "sec"),
        P("col", None),
        P("col", None),
        P("col", None),
        P("col", None, None),
    )
    return jax.shard_map(
        absorb_row,
        mesh=mesh,
        in_specs=placed,
        out_specs=(P("col", "sec", None, None, None), P()),
        check_vma=False,
    )
```

```python
import functools

import jax
import jax.numpy as jnp
import numpy as np
from jax import lax
from jax.experimental import pallas as pl
from jax.experimental.pallas import tpu as pltpu
from jax.sharding import PartitionSpec as P

LANES = 128
QUAD = 4
VMEM_LIMIT = 36 << 20
FRONT_FLOPS = 1 << 30


def round_up(value, multiple):
    return -(-value // multiple) * multiple


def from_behind(x, axis, by):
    count = lax.axis_size(axis)
    return lax.ppermute(x, axis, [(i, (i + by) % count) for i in range(count)])


class Plan:
    def __init__(self, chi, half, legs, phys):
        self.chi, self.half, self.legs, self.phys = chi, half, legs, phys
        self.lanes = round_up(chi, LANES)
        self.lm = round_up(legs * legs, 8)
        self.pairs = legs // 2
        self.group_rows = 2 * legs * phys
        self.groups = legs * self.pairs
        self.rows2 = self.groups * self.group_rows
        self.cols2 = round_up(legs * self.lm, 256)
        self.seg = 2 * legs
        self.rows3 = round_up(legs * self.seg, 16)
        self.cols3 = legs * self.group_rows
        self.xrows = self.pairs * self.seg

    def matrices(self):
        n, ph = self.legs, self.phys
        wide = n * n * ph
        r2 = np.zeros((self.rows2, wide), np.float32)
        row_m = np.zeros((self.rows2,), np.int64)
        for r in range(n):
            for d in range(n):
                for m in range(n):
                    for p in range(ph):
                        g = r * self.pairs + d // 2
                        row = g * self.group_rows + (d % 2) * n * ph + m * ph + p
                        r2[row, (d * ph + p) * n + r] = 1
                        row_m[row] = m
        c2 = np.zeros((n * n, self.cols2), np.float32)
        col_m = np.full((self.cols2,), -1)
        for u in range(n):
            for l in range(n):
                for m in range(n):
                    c = u * self.lm + l * n + m
                    c2[u * n + l, c] = 1
                    col_m[c] = m
        m2 = row_m[:, None] == col_m[None, :]
        r3 = np.zeros((ph, self.rows3, wide), np.float32)
        row_d = np.full((self.rows3,), -1)
        for s in range(n):
            for d2 in range(2):
                for e in range(n):
                    row = s * self.seg + d2 * n + e
                    row_d[row] = d2
                    for p in range(ph):
                        r3[p, row, (e * ph + p) * n + s] = 1
        c3 = np.zeros((ph, n * n, self.cols3), np.float32)
        col_d = np.zeros((self.cols3,), np.int64)
        for v in range(n):
            for d2 in range(2):
                for m in range(n):
                    for p in range(ph):
                        col = v * self.group_rows + d2 * n * ph + m * ph + p
                        c3[p, v * n + m, col] = 1
                        col_d[col] = d2
        m3 = row_d[:, None] == col_d[None, :]
        return [jnp.asarray(x, jnp.bfloat16) for x in (r2, c2, m2, r3, c3, m3)]

    def indices(self):
        n, ph = self.legs, self.phys
        rows = np.zeros((max(n * n * ph, self.rows3), 8), np.int32)
        cols = np.zeros((8, self.cols2), np.int32)
        for i in range(n * n * ph):
            rest = i % self.group_rows
            rows[i, 0] = i // self.group_rows * 2 + rest // (n * ph)
            rows[i, 1] = rest % ph
        for i in range(self.rows3):
            rows[i, 2] = i % n
        for u in range(n):
            for i in range(n * n):
                cols[:2, u * self.lm + i] = u, i // n
        for i in range(self.cols3):
            rest = i % (n * ph)
            cols[2:5, i] = i // self.group_rows, rest // ph, rest % ph
        return [jnp.asarray(rows), jnp.asarray(cols)]


def column_of(row):
    square = (row.shape[1], row.shape[1])
    diagonal = lax.broadcasted_iota(jnp.int32, square, 0) == lax.broadcasted_iota(jnp.int32, square, 1)
    return jnp.sum(jnp.where(diagonal, jnp.broadcast_to(row, square), 0), axis=1, keepdims=True)


def look_up(index, table):
    out = jnp.zeros(index.shape, jnp.int32)
    for k, value in enumerate(table):
        out = out + jnp.where(index == k, value, 0)
    return out


def dot(a, b):
    return jnp.dot(a, b, preferred_element_type=jnp.float32)


def fetch(pairs, sems):
    copies = [pltpu.make_async_copy(src, dst, sems.at[i]) for i, (src, dst) in enumerate(pairs)]
    for copy in copies:
        copy.start()
    return copies


def prep_kernel(
    plan,
    ket, left_h, bond_h, fresh_h, link_h, vert_h, r2_h, c2_h, m2_h, r3_h, c3_h, m3_h, rows_h, cols_h,
    out, k2, k3, gap2, gap3, bond_col,
    wide, left, bond, fresh, link_s, vert_s, r2, c2, m2, r3, c3, m3, rows, cols, sems,
):
    n, half, lm = plan.legs, plan.half, plan.lm
    sources = (link_h, vert_h, bond_h, fresh_h, left_h, r2_h, c2_h, m2_h, r3_h, c3_h, m3_h, rows_h, cols_h)
    targets = (link_s, vert_s, bond, fresh, left, r2, c2, m2, r3, c3, m3, rows, cols)
    copies = fetch(list(zip(sources, targets)), sems)
    for row in range(n * n, lm):
        wide[pl.ds(row, half, stride=lm), :] = jnp.zeros((half, plan.chi), jnp.float32)
    for copy in copies[:5]:
        copy.wait()
    sec = lax.axis_index("sec")
    link = [link_s[0, i] for i in range(n)]
    upper = [vert_s[0, 0, i] for i in range(n)]
    lower = [vert_s[0, 1, i] for i in range(n)]
    fresh_all = column_of(fresh[...])
    fresh_col = jnp.where(sec == 0, fresh_all[:half], fresh_all[half:])
    bond_col[...] = column_of(bond[...])
    gap = fresh_col - bond[...]
    for l in range(n):
        for m in range(n):
            keep = gap == link[l] - link[m]
            val = jnp.where(keep, left[l * n + m].astype(jnp.float32), 0.0)
            wide[pl.ds(l * n + m, half, stride=lm), :] = val
    out[...] = wide[...].astype(jnp.bfloat16)
    for copy in copies[5:]:
        copy.wait()

    def expand(first, second):
        picked = lax.dot_general(first, ket[...], (((1,), (1,)), ((), ())), preferred_element_type=jnp.float32)
        return dot(picked.astype(jnp.bfloat16), second)

    k2[...] = (expand(r2[...], c2[...]) * m2[...].astype(jnp.float32)).astype(jnp.bfloat16)
    total = expand(r3[0], c3[0])
    for p in range(1, plan.phys):
        total = total + expand(r3[p], c3[p])
    k3[...] = (total * m3[...].astype(jnp.float32)).astype(jnp.bfloat16)
    tall = n * n * plan.phys
    rows_d = look_up(rows[:tall, 0:1], lower) + rows[:tall, 1:2]
    gap2[...] = look_up(cols[0:1, :], upper) + look_up(cols[1:2, :], link) - rows_d
    rows_e = look_up(rows[: plan.rows3, 2:3], lower)
    c = slice(0, plan.cols3)
    gap3[...] = look_up(cols[2:3, c], upper) + look_up(cols[3:4, c], link) - cols[4:5, c] - rows_e


def halves(first, second):
    sec = lax.axis_index("sec")
    return ((first, sec), (second, 1 - sec))


def pack_lanes(parts, chi):
    lane = lax.broadcasted_iota(jnp.int32, parts[0].shape, 1)
    tiles = []
    for x, part in enumerate(parts):
        first, shift = divmod(x * chi, LANES)
        rolled = pltpu.roll(part, shift, 1) if shift else part
        if first == len(tiles):
            tiles.append(rolled)
        else:
            tiles[first] = jnp.where(lane < shift, tiles[first], rolled)
        if shift + chi > LANES:
            tiles.append(rolled)
    return tiles


def unpack_lanes(tiles, chi, count):
    lane = lax.broadcasted_iota(jnp.int32, tiles[0].shape, 1)
    parts = []
    for x in range(count):
        first, shift = divmod(x * chi, LANES)
        part = tiles[first]
        if shift + chi > LANES:
            part = jnp.where(lane >= shift, part, tiles[first + 1])
        parts.append(pltpu.roll(part, LANES - shift, 1) if shift else part)
    return parts


def first(plan, left, ms, w1, vp):
    chi, lm = plan.chi, plan.lm
    for up in range(plan.pairs):
        both = dot(left, ms[up, vp])
        for k in range(2):
            parts = []
            for x in range(QUAD):
                rows = both[x * lm : (x + 1) * lm]
                parts.append(
                    jnp.concatenate([rows[:, c * LANES : (c + 1) * LANES] for c in (2 * k, 2 * k + 1)], axis=0)
                )
            for t, tile in enumerate(pack_lanes(parts, chi)):
                at = (2 * t + k) * LANES
                w1[vp, up * 2 * lm : (up + 1) * 2 * lm, at : at + LANES] = tile.astype(jnp.bfloat16)


def second(plan, k2, w1, w2, vp, half_of_oct):
    gr, wide = plan.group_rows, QUAD * plan.chi
    out = dot(k2[...], w1[vp])
    for g in range(plan.groups):
        part = out[g * gr : (g + 1) * gr]
        for t in range(wide // LANES):
            pair = [part[:, c * LANES : (c + 1) * LANES] for c in (2 * t, 2 * t + 1)]
            at = half_of_oct * wide + t * LANES
            w2[g, vp * 2 * gr : (vp + 1) * 2 * gr, at : at + LANES] = jnp.concatenate(pair, axis=0).astype(jnp.bfloat16)


def third(plan, k3, w2, w3, g):
    seg = plan.seg
    r, dp = g // plan.pairs, g % plan.pairs
    out = dot(k3[...], w2[g])
    per = QUAD * plan.chi // LANES
    quad = QUAD * plan.xrows
    for h in range(2):
        tiles = [out[:, t * LANES : (t + 1) * LANES] for t in range(h * per, (h + 1) * per)]
        parts = unpack_lanes(tiles, plan.chi, QUAD)
        at = h * quad + dp * QUAD * seg
        for s in range(plan.legs):
            stacked = jnp.concatenate([part[s * seg : (s + 1) * seg] for part in parts], axis=0)
            w3[r, at : at + QUAD * seg, s * LANES : (s + 1) * LANES] = stacked.astype(jnp.bfloat16)


def fourth(w3, pr, r):
    return lax.dot_general(w3[r], pr[r], (((1,), (1,)), ((), ())), preferred_element_type=jnp.float32)


def add(total, term):
    return term if total is None else total + term


def quad_rows(lhs, plan, quad):
    rows = QUAD * plan.lm
    return lhs[pl.ds(pl.multiple_of(quad * rows, 16), rows), :]


def front_kernel(
    plan,
    charges_s, charges_v, other, lhs, k2_all, k3_all, gap2, gap3, bond_col, mine_h, vert_h,
    ms, k2, k3, w2, w3_a, w3_b,
    w1, w2_a, w2_b, mine, vert_s, sems,
):
    n, chi, half, lanes = plan.legs, plan.chi, plan.half, plan.lanes
    bf16 = jnp.bfloat16
    copies = fetch([(vert_h, vert_s), (mine_h, mine)], sems)
    link_next = [charges_s[2, i] for i in range(n)]
    bond_next = charges_v[0:1, :]
    tall = plan.pairs * plan.group_rows
    for r in range(n):
        at = slice(r * tall, (r + 1) * tall)
        k2[at] = jnp.where(gap2[...] == link_next[r], k2_all[at].astype(jnp.float32), 0.0).astype(bf16)
    row = lax.broadcasted_iota(jnp.int32, gap3.shape, 0)
    link_rows = jnp.zeros(gap3.shape, jnp.int32)
    for s in range(n):
        link_rows = jnp.where(row >= s * plan.seg, link_next[s], link_rows)
    k3[...] = jnp.where(gap3[...] == link_rows, k3_all[...].astype(jnp.float32), 0.0).astype(bf16)
    if chi < lanes:
        for k in range(4):
            at = slice(k * lanes + chi, (k + 1) * lanes)
            ms[:, :, :, at] = jnp.zeros((plan.pairs, plan.pairs, chi, lanes - chi), bf16)
    copies[0].wait()
    upper = [vert_s[0, 0, i] for i in range(n)]
    copies[1].wait()
    for src, which in halves(mine, other):
        at = pl.multiple_of(which * half, 16)
        gap = bond_next - bond_col[pl.ds(at, half), :]
        for u in range(n):
            for v in range(n):
                keep = gap == upper[u] - upper[v]
                val = jnp.where(keep, src[u * n + v].astype(jnp.float32), 0.0)
                lane = (v % 2 * 2 + u % 2) * lanes
                ms[u // 2, v // 2, pl.ds(at, half), lane : lane + chi] = val.astype(bf16)
    pad = n * plan.lm
    w1[:, :, pad:, :] = jnp.zeros((2, plan.pairs, plan.cols2 - pad, w1.shape[3]), bf16)
    phases = [(o, vp, h) for o in range(3) for vp in range(plan.pairs) for h in range(2)]
    per_g = plan.groups // (2 * plan.pairs)
    chain, done = (w2_a, w2_b, w2), (w3_a, w3_b)

    def lead(o, vp, h):
        first(plan, quad_rows(lhs, plan, 2 * o + h), ms, w1.at[h], vp)

    lead(*phases[0])
    for i, (o, vp, h) in enumerate(phases):
        if i + 1 < len(phases):
            lead(*phases[i + 1])
        if o:
            at = (2 * vp + h) * per_g
            for g in range(at, at + per_g):
                third(plan, k3, chain[o - 1], done[o - 1], g)
        second(plan, k2, w1.at[h], chain[o], vp, h)


def middle_kernel(plan, lhs, ms, k2, k3, w2_in, w2, w3, w1):
    pad = plan.legs * plan.lm
    w1[:, :, pad:, :] = jnp.zeros((2, plan.pairs, plan.cols2 - pad, w1.shape[3]), jnp.bfloat16)
    phases = [(vp, h) for vp in range(plan.pairs) for h in range(2)]
    per_g = plan.groups // len(phases)

    def lead(vp, h):
        first(plan, quad_rows(lhs, plan, 6 + h), ms, w1.at[h], vp)

    lead(*phases[0])
    for i, (vp, h) in enumerate(phases):
        if i + 1 < len(phases):
            lead(*phases[i + 1])
        for g in range(i * per_g, (i + 1) * per_g):
            third(plan, k3, w2_in, w3, g)
        second(plan, k2, w1.at[h], w2, vp, h)


def back_kernel(
    plan,
    charges_s,
    charges_v, lhs, ms, k2, k3, w2_in, w3_a, w3_b, w3_c, pr_mine, pr_other,
    image, partial,
    pr, w1, w2_a, w2_b, w3_d, w3_e, w3_f,
):
    n, chi, half, lanes = plan.legs, plan.chi, plan.half, plan.lanes
    bf16 = jnp.bfloat16
    link_next = [charges_s[2, i] for i in range(n)]
    bond_next = charges_v[0:1, :]
    fresh_col = column_of(charges_v[1:2, :])
    pr[...] = jnp.zeros_like(pr)
    for src, which in halves(pr_mine, pr_other):
        at = pl.multiple_of(which * half, 16)
        gap = jnp.where(which == 0, fresh_col[:half], fresh_col[half:]) - bond_next
        for r in range(n):
            for s in range(n):
                keep = gap == link_next[r] - link_next[s]
                val = jnp.where(keep, src[r * n + s].astype(jnp.float32), 0.0)
                pr[r, pl.ds(at, half), s * lanes : s * lanes + chi] = val.astype(bf16)
    pad = n * plan.lm
    w1[:, :, pad:, :] = jnp.zeros((2, plan.pairs, plan.cols2 - pad, w1.shape[3]), bf16)

    block = 2 * QUAD * plan.xrows
    per_g = plan.groups // (2 * plan.pairs)
    per_r = n // (2 * plan.pairs)

    def put(oct, total):
        pieces = []
        for h in range(2):
            for x in range(QUAD):
                for dp in range(plan.pairs):
                    at = ((h * plan.pairs + dp) * QUAD + x) * plan.seg
                    pieces.append(total[at : at + plan.seg])
        image[oct * block : (oct + 1) * block, :] = jnp.concatenate(pieces, axis=0)
        return jnp.sum(total * total)

    w2 = (w2_in, w2_a, w2_b)
    w3 = (w3_a, w3_b, w3_c, w3_d, w3_e, w3_f)
    phases = [(o, vp, h) for o in range(2) for vp in range(plan.pairs) for h in range(2)]

    def lead(o, vp, h):
        first(plan, quad_rows(lhs, plan, 2 * (o + 4) + h), ms, w1.at[h], vp)

    square_sum = 0.0
    total = None
    lead(*phases[0])
    for i, (o, vp, h) in enumerate(phases):
        if i + 1 < len(phases):
            lead(*phases[i + 1])
        phase = 2 * vp + h
        for g in range(phase * per_g, (phase + 1) * per_g):
            third(plan, k3, w2[o], w3[o + 3], g)
        for r in range(phase * per_r, (phase + 1) * per_r):
            total = add(total, fourth(w3[o], pr, r))
        second(plan, k2, w1.at[h], w2[o + 1], vp, h)
        if phase == 2 * plan.pairs - 1:
            square_sum = square_sum + put(o, total)
            total = None
    partial[...] = jnp.full_like(partial, square_sum)

    @pl.when(lax.axis_index("sec") >= 0)
    def _():
        square_sum = 0.0
        total = None
        for g in range(plan.groups):
            third(plan, k3, w2[2], w3[5], g)
            if g % plan.pairs == 0:
                total = add(total, fourth(w3[2], pr, g // plan.pairs))
        square_sum = square_sum + put(2, total)
        for o in range(3, 6):
            even = odd = None
            for r in range(0, n, 2):
                even = add(even, fourth(w3[o], pr, r))
                odd = add(odd, fourth(w3[o], pr, r + 1))
            square_sum = square_sum + put(o, even + odd)
        partial[...] += jnp.full_like(partial, square_sum)


def finish_kernel(plan, count, columns, incoming, image, new, log_norm):
    n, half = plan.legs, plan.half
    sums = incoming[...]
    devices = sums.shape[0]
    row = lax.broadcasted_iota(jnp.int32, sums.shape, 0)
    pair = sums + pltpu.roll(sums, devices - 1, 0)
    logs = 0.5 * jnp.log(pair / count + 1e-06)
    log_norm[0, 0] = jnp.sum(jnp.where(row % 2 == 0, logs, 0.0)[:, :1]) / columns
    here = jnp.sum(jnp.where(row == 2 * lax.axis_index("col"), pair, 0.0), axis=0, keepdims=True)
    scale = lax.rsqrt(here / count + 1e-06)[:, : plan.chi]
    for d in range(n):
        for e in range(n):
            at = (d // 2) * plan.seg + (d % 2) * n + e
            new[d * n + e] = (image[pl.ds(at, half, stride=plan.xrows), :] * scale).astype(jnp.bfloat16)


def whole(memory, count):
    return [pl.BlockSpec(memory_space=memory) for _ in range(count)]


def absorb_row(mps, ket, left_proj, right_proj, bond_charge, new_charge, link_charge, vert_charge):
    half, chi, legs = left_proj.shape[1], left_proj.shape[2], left_proj.shape[3]
    phys = ket.shape[5]
    plan = Plan(chi, half, legs, phys)
    squared = legs * legs
    columns, sections = lax.axis_size("col"), lax.axis_size("sec")
    bf16, f32 = jnp.bfloat16, jnp.float32
    smem, vmem = pltpu.SMEM, pltpu.VMEM
    swap = [(i, 1 - i) for i in range(sections)]
    hbm = pltpu.HBM
    link_row = jnp.pad(link_charge, ((0, 0), (0, chi - legs)))
    charges = from_behind(jnp.concatenate([bond_charge, new_charge, link_row], axis=0), "col", -1)
    mine = jnp.transpose(mps[0], (1, 2, 0, 3)).reshape(squared, half, chi)
    other = lax.ppermute(mine, "sec", swap)
    pr_mine = from_behind(jnp.transpose(right_proj[0], (1, 2, 3, 0)).reshape(squared, half, chi), "col", -1)
    left = jnp.transpose(left_proj[0], (2, 3, 0, 1)).reshape(squared, half, chi)
    flat_ket = jnp.transpose(ket[0], (0, 1, 2, 4, 3)).reshape(squared, squared * phys)
    fetched = [left, bond_charge, new_charge, link_charge, vert_charge] + plan.matrices() + plan.indices()
    in_smem = (3, 4)
    scratch = [(smem if i in in_smem else vmem)(x.shape, x.dtype) for i, x in enumerate(fetched)]
    scratch = [scratch[i] for i in (0, 1, 2, 3, 4)] + scratch[5:]
    lhs, *kets = pl.pallas_call(
        functools.partial(prep_kernel, plan),
        in_specs=whole(vmem, 1) + whole(hbm, len(fetched)),
        out_specs=whole(vmem, 6),
        out_shape=[
            jax.ShapeDtypeStruct((half * plan.lm, chi), bf16),
            jax.ShapeDtypeStruct((plan.rows2, plan.cols2), bf16),
            jax.ShapeDtypeStruct((plan.rows3, plan.cols3), bf16),
            jax.ShapeDtypeStruct((squared * phys, plan.cols2), jnp.int32),
            jax.ShapeDtypeStruct((plan.rows3, plan.cols3), jnp.int32),
            jax.ShapeDtypeStruct((chi, 1), jnp.int32),
        ],
        scratch_shapes=[pltpu.VMEM((half * plan.lm, chi), f32)] + scratch + [pltpu.SemaphoreType.DMA((len(fetched),))],
        compiler_params=pltpu.CompilerParams(vmem_limit_bytes=12 << 20),
        cost_estimate=pl.CostEstimate(flops=FRONT_FLOPS // 8, bytes_accessed=1 << 20, transcendentals=0),
        name="prep",
    )(flat_ket, *[pltpu.with_memory_space_constraint(x, pltpu.HBM) for x in fetched])
    octs = half // (2 * QUAD)
    if half % (2 * QUAD) or octs != 6 or (QUAD * chi) % LANES or QUAD * plan.seg % 16:
        raise ValueError("half")
    block = 2 * QUAD * plan.xrows
    lanes = plan.lanes
    wide = 2 * QUAD * chi
    w1_shape = (2, plan.pairs, plan.cols2, wide)
    w2_shape = jax.ShapeDtypeStruct((plan.groups, plan.cols3, wide), bf16)
    w3_shape = jax.ShapeDtypeStruct((legs, block, legs * lanes), bf16)
    operands = [charges, charges, other, lhs] + kets
    operands += [pltpu.with_memory_space_constraint(x, pltpu.HBM) for x in (mine, vert_charge)]
    ms, k2, k3, w2, *w3 = pl.pallas_call(
        functools.partial(front_kernel, plan),
        in_specs=whole(smem, 1) + whole(vmem, len(operands) - 3) + whole(hbm, 2),
        out_specs=whole(vmem, 6),
        out_shape=[
            jax.ShapeDtypeStruct((plan.pairs, plan.pairs, chi, 4 * lanes), bf16),
            jax.ShapeDtypeStruct((plan.rows2, plan.cols2), bf16),
            jax.ShapeDtypeStruct((plan.rows3, plan.cols3), bf16),
            w2_shape,
            w3_shape,
            w3_shape,
        ],
        scratch_shapes=[
            pltpu.VMEM(w1_shape, bf16),
            pltpu.VMEM(w2_shape.shape, bf16),
            pltpu.VMEM(w2_shape.shape, bf16),
            pltpu.VMEM(mine.shape, bf16),
            pltpu.SMEM(vert_charge.shape, jnp.int32),
            pltpu.SemaphoreType.DMA((2,)),
        ],
        compiler_params=pltpu.CompilerParams(vmem_limit_bytes=VMEM_LIMIT),
        cost_estimate=pl.CostEstimate(flops=FRONT_FLOPS, bytes_accessed=1 << 20, transcendentals=0),
        name="front",
    )(*operands)
    pr_mine, w2 = lax.optimization_barrier((pr_mine, w2))
    pr_other = lax.ppermute(pr_mine, "sec", swap)
    w2, w3_last = pl.pallas_call(
        functools.partial(middle_kernel, plan),
        in_specs=whole(vmem, 5),
        out_specs=whole(vmem, 2),
        out_shape=[w2_shape, w3_shape],
        scratch_shapes=[pltpu.VMEM(w1_shape, bf16)],
        compiler_params=pltpu.CompilerParams(vmem_limit_bytes=20 << 20),
        cost_estimate=pl.CostEstimate(flops=FRONT_FLOPS, bytes_accessed=1 << 20, transcendentals=0),
        name="middle",
    )(lhs, ms, k2, k3, w2)
    operands = [charges, charges, lhs, ms, k2, k3, w2, *w3, w3_last, pr_mine, pr_other]
    image, partial = pl.pallas_call(
        functools.partial(back_kernel, plan),
        in_specs=whole(smem, 1) + whole(vmem, len(operands) - 1),
        out_specs=whole(vmem, 2),
        out_shape=[
            jax.ShapeDtypeStruct((octs * block, chi), f32),
            jax.ShapeDtypeStruct((columns * sections, 1, LANES), f32),
        ],
        scratch_shapes=[
            pltpu.VMEM((legs, chi, legs * lanes), bf16),
            pltpu.VMEM(w1_shape, bf16),
        ]
        + [pltpu.VMEM(w2_shape.shape, bf16)] * 2
        + [pltpu.VMEM(w3_shape.shape, bf16)] * 3,
        compiler_params=pltpu.CompilerParams(vmem_limit_bytes=VMEM_LIMIT),
        cost_estimate=pl.CostEstimate(flops=2 * FRONT_FLOPS, bytes_accessed=1 << 20, transcendentals=0),
        name="back",
    )(*operands)
    incoming = lax.all_to_all(partial, ("col", "sec"), 0, 0, tiled=True)
    new, log_norm = pl.pallas_call(
        functools.partial(finish_kernel, plan, float(chi * squared * chi), float(columns)),
        in_specs=whole(vmem, 2),
        out_specs=whole(vmem, 1) + whole(smem, 1),
        out_shape=[
            jax.ShapeDtypeStruct((squared, half, chi), bf16),
            jax.ShapeDtypeStruct((1, 1), f32),
        ],
        compiler_params=pltpu.CompilerParams(vmem_limit_bytes=8 << 20),
        name="finish",
    )(incoming.reshape(columns * sections, LANES), image)
    new_mps = jnp.transpose(new.reshape(legs, legs, half, chi), (2, 0, 1, 3))[None]
    return (new_mps, log_norm.reshape(()))


def solution(mesh):
    placed = (
        P("col", "sec", None, None, None),
        P("col", None, None, None, None, None),
        P("col", "sec", None, None, None),
        P("col", None, None, None, "sec"),
        P("col", None),
        P("col", None),
        P("col", None),
        P("col", None, None),
    )
    return jax.shard_map(
        absorb_row,
        mesh=mesh,
        in_specs=placed,
        out_specs=(P("col", "sec", None, None, None), P()),
        check_vma=False,
    )
```

```python
import functools

import jax
import jax.numpy as jnp
import numpy as np
from jax import lax
from jax.experimental import pallas as pl
from jax.experimental.pallas import tpu as pltpu
from jax.sharding import PartitionSpec as P

LANES = 128
QUAD = 4
VMEM_LIMIT = 36 << 20
FRONT_FLOPS = 1 << 30


def round_up(value, multiple):
    return -(-value // multiple) * multiple


def from_behind(x, axis, by):
    count = lax.axis_size(axis)
    return lax.ppermute(x, axis, [(i, (i + by) % count) for i in range(count)])


class Plan:
    def __init__(self, chi, half, legs, phys):
        self.chi, self.half, self.legs, self.phys = chi, half, legs, phys
        self.lanes = round_up(chi, LANES)
        self.lm = round_up(legs * legs, 8)
        self.pairs = legs // 2
        self.group_rows = 2 * legs * phys
        self.groups = legs * self.pairs
        self.rows2 = self.groups * self.group_rows
        self.cols2 = round_up(legs * self.lm, 256)
        self.seg = 2 * legs
        self.rows3 = round_up(legs * self.seg, 16)
        self.cols3 = legs * self.group_rows
        self.xrows = self.pairs * self.seg

    def matrices(self):
        n, ph = self.legs, self.phys
        wide = n * n * ph
        r2 = np.zeros((self.rows2, wide), np.float32)
        row_m = np.zeros((self.rows2,), np.int64)
        for r in range(n):
            for d in range(n):
                for m in range(n):
                    for p in range(ph):
                        g = r * self.pairs + d // 2
                        row = g * self.group_rows + (d % 2) * n * ph + m * ph + p
                        r2[row, (d * ph + p) * n + r] = 1
                        row_m[row] = m
        c2 = np.zeros((n * n, self.cols2), np.float32)
        col_m = np.full((self.cols2,), -1)
        for u in range(n):
            for l in range(n):
                for m in range(n):
                    c = u * self.lm + l * n + m
                    c2[u * n + l, c] = 1
                    col_m[c] = m
        m2 = row_m[:, None] == col_m[None, :]
        r3 = np.zeros((ph, self.rows3, wide), np.float32)
        row_d = np.full((self.rows3,), -1)
        for s in range(n):
            for d2 in range(2):
                for e in range(n):
                    row = s * self.seg + d2 * n + e
                    row_d[row] = d2
                    for p in range(ph):
                        r3[p, row, (e * ph + p) * n + s] = 1
        c3 = np.zeros((ph, n * n, self.cols3), np.float32)
        col_d = np.zeros((self.cols3,), np.int64)
        for v in range(n):
            for d2 in range(2):
                for m in range(n):
                    for p in range(ph):
                        col = v * self.group_rows + d2 * n * ph + m * ph + p
                        c3[p, v * n + m, col] = 1
                        col_d[col] = d2
        m3 = row_d[:, None] == col_d[None, :]
        return [jnp.asarray(x, jnp.bfloat16) for x in (r2, c2, m2, r3, c3, m3)]

    def indices(self):
        n, ph = self.legs, self.phys
        rows = np.zeros((max(n * n * ph, self.rows3), 8), np.int32)
        cols = np.zeros((8, self.cols2), np.int32)
        for i in range(n * n * ph):
            rest = i % self.group_rows
            rows[i, 0] = i // self.group_rows * 2 + rest // (n * ph)
            rows[i, 1] = rest % ph
        for i in range(self.rows3):
            rows[i, 2] = i % n
        for u in range(n):
            for i in range(n * n):
                cols[:2, u * self.lm + i] = u, i // n
        for i in range(self.cols3):
            rest = i % (n * ph)
            cols[2:5, i] = i // self.group_rows, rest // ph, rest % ph
        return [jnp.asarray(rows), jnp.asarray(cols)]


def column_of(row):
    square = (row.shape[1], row.shape[1])
    diagonal = lax.broadcasted_iota(jnp.int32, square, 0) == lax.broadcasted_iota(jnp.int32, square, 1)
    return jnp.sum(jnp.where(diagonal, jnp.broadcast_to(row, square), 0), axis=1, keepdims=True)


def look_up(index, table):
    out = jnp.zeros(index.shape, jnp.int32)
    for k, value in enumerate(table):
        out = out + jnp.where(index == k, value, 0)
    return out


def dot(a, b):
    return jnp.dot(a, b, preferred_element_type=jnp.float32)


def fetch(pairs, sems):
    copies = [pltpu.make_async_copy(src, dst, sems.at[i]) for i, (src, dst) in enumerate(pairs)]
    for copy in copies:
        copy.start()
    return copies


def prep_kernel(
    plan,
    ket, left_h, bond_h, fresh_h, link_h, vert_h, r2_h, c2_h, m2_h, r3_h, c3_h, m3_h, rows_h, cols_h, mine_h,
    out, k2, k3, gap2, gap3, bond_col, upper_rows, mine,
    wide, left, bond, fresh, link_s, vert_s, r2, c2, m2, r3, c3, m3, rows, cols, sems,
):
    n, half, lm = plan.legs, plan.half, plan.lm
    sources = (link_h, vert_h, bond_h, fresh_h, left_h, r2_h, c2_h, m2_h, r3_h, c3_h, m3_h, rows_h, cols_h, mine_h)
    targets = (link_s, vert_s, bond, fresh, left, r2, c2, m2, r3, c3, m3, rows, cols, mine)
    copies = fetch(list(zip(sources, targets)), sems)
    for row in range(n * n, lm):
        wide[pl.ds(row, half, stride=lm), :] = jnp.zeros((half, plan.chi), jnp.float32)
    for copy in copies[:5]:
        copy.wait()
    sec = lax.axis_index("sec")
    link = [link_s[0, i] for i in range(n)]
    upper = [vert_s[0, 0, i] for i in range(n)]
    lower = [vert_s[0, 1, i] for i in range(n)]
    fresh_all = column_of(fresh[...])
    fresh_col = jnp.where(sec == 0, fresh_all[:half], fresh_all[half:])
    bond_col[...] = column_of(bond[...])
    for i in range(n):
        upper_rows[i : i + 1, :] = jnp.full((1, plan.chi), upper[i], jnp.int32)
    gap = fresh_col - bond[...]
    for l in range(n):
        for m in range(n):
            keep = gap == link[l] - link[m]
            val = jnp.where(keep, left[l * n + m].astype(jnp.float32), 0.0)
            wide[pl.ds(l * n + m, half, stride=lm), :] = val
    out[...] = wide[...].astype(jnp.bfloat16)
    for copy in copies[5:]:
        copy.wait()

    def expand(first, second):
        picked = lax.dot_general(first, ket[...], (((1,), (1,)), ((), ())), preferred_element_type=jnp.float32)
        return dot(picked.astype(jnp.bfloat16), second)

    k2[...] = (expand(r2[...], c2[...]) * m2[...].astype(jnp.float32)).astype(jnp.bfloat16)
    total = expand(r3[0], c3[0])
    for p in range(1, plan.phys):
        total = total + expand(r3[p], c3[p])
    k3[...] = (total * m3[...].astype(jnp.float32)).astype(jnp.bfloat16)
    tall = n * n * plan.phys
    rows_d = look_up(rows[:tall, 0:1], lower) + rows[:tall, 1:2]
    gap2[...] = look_up(cols[0:1, :], upper) + look_up(cols[1:2, :], link) - rows_d
    rows_e = look_up(rows[: plan.rows3, 2:3], lower)
    c = slice(0, plan.cols3)
    gap3[...] = look_up(cols[2:3, c], upper) + look_up(cols[3:4, c], link) - cols[4:5, c] - rows_e


def halves(first, second):
    sec = lax.axis_index("sec")
    return ((first, sec), (second, 1 - sec))


def pack_lanes(parts, chi):
    lane = lax.broadcasted_iota(jnp.int32, parts[0].shape, 1)
    tiles = []
    for x, part in enumerate(parts):
        first, shift = divmod(x * chi, LANES)
        rolled = pltpu.roll(part, shift, 1) if shift else part
        if first == len(tiles):
            tiles.append(rolled)
        else:
            tiles[first] = jnp.where(lane < shift, tiles[first], rolled)
        if shift + chi > LANES:
            tiles.append(rolled)
    return tiles


def unpack_lanes(tiles, chi, count):
    lane = lax.broadcasted_iota(jnp.int32, tiles[0].shape, 1)
    parts = []
    for x in range(count):
        first, shift = divmod(x * chi, LANES)
        part = tiles[first]
        if shift + chi > LANES:
            part = jnp.where(lane >= shift, part, tiles[first + 1])
        parts.append(pltpu.roll(part, LANES - shift, 1) if shift else part)
    return parts


def first(plan, left, ms, w1, vp):
    chi, lm = plan.chi, plan.lm
    for up in range(plan.pairs):
        both = dot(left, ms[up, vp])
        for k in range(2):
            parts = []
            for x in range(QUAD):
                rows = both[x * lm : (x + 1) * lm]
                parts.append(
                    jnp.concatenate([rows[:, c * LANES : (c + 1) * LANES] for c in (2 * k, 2 * k + 1)], axis=0)
                )
            for t, tile in enumerate(pack_lanes(parts, chi)):
                at = (2 * t + k) * LANES
                w1[vp, up * 2 * lm : (up + 1) * 2 * lm, at : at + LANES] = tile.astype(jnp.bfloat16)


def second(plan, k2, w1, w2, vp, half_of_oct):
    gr, wide = plan.group_rows, QUAD * plan.chi
    out = dot(k2[...], w1[vp])
    for g in range(plan.groups):
        part = out[g * gr : (g + 1) * gr]
        for t in range(wide // LANES):
            pair = [part[:, c * LANES : (c + 1) * LANES] for c in (2 * t, 2 * t + 1)]
            at = half_of_oct * wide + t * LANES
            w2[g, vp * 2 * gr : (vp + 1) * 2 * gr, at : at + LANES] = jnp.concatenate(pair, axis=0).astype(jnp.bfloat16)


def third(plan, k3, w2, w3, g):
    seg = plan.seg
    r, dp = g // plan.pairs, g % plan.pairs
    out = dot(k3[...], w2[g])
    per = QUAD * plan.chi // LANES
    quad = QUAD * plan.xrows
    for h in range(2):
        tiles = [out[:, t * LANES : (t + 1) * LANES] for t in range(h * per, (h + 1) * per)]
        parts = unpack_lanes(tiles, plan.chi, QUAD)
        at = h * quad + dp * QUAD * seg
        for s in range(plan.legs):
            stacked = jnp.concatenate([part[s * seg : (s + 1) * seg] for part in parts], axis=0)
            w3[r, at : at + QUAD * seg, s * LANES : (s + 1) * LANES] = stacked.astype(jnp.bfloat16)


def fourth(w3, pr, r):
    return lax.dot_general(w3[r], pr[r], (((1,), (1,)), ((), ())), preferred_element_type=jnp.float32)


def add(total, term):
    return term if total is None else total + term


def quad_rows(lhs, plan, quad):
    rows = QUAD * plan.lm
    return lhs[pl.ds(pl.multiple_of(quad * rows, 16), rows), :]


def front_kernel(
    plan,
    charges_s, charges_v, other, lhs, k2_all, k3_all, gap2, gap3, bond_col, upper_rows, mine,
    ms, k2, k3, w2, w3_a, w3_b,
    w1, w2_a, w2_b,
):
    n, chi, half, lanes = plan.legs, plan.chi, plan.half, plan.lanes
    bf16 = jnp.bfloat16
    link_next = [charges_s[2, i] for i in range(n)]
    bond_next = charges_v[0:1, :]
    tall = plan.pairs * plan.group_rows
    for r in range(n):
        at = slice(r * tall, (r + 1) * tall)
        k2[at] = jnp.where(gap2[...] == link_next[r], k2_all[at].astype(jnp.float32), 0.0).astype(bf16)
    row = lax.broadcasted_iota(jnp.int32, gap3.shape, 0)
    link_rows = jnp.zeros(gap3.shape, jnp.int32)
    for s in range(n):
        link_rows = jnp.where(row >= s * plan.seg, link_next[s], link_rows)
    k3[...] = jnp.where(gap3[...] == link_rows, k3_all[...].astype(jnp.float32), 0.0).astype(bf16)
    if chi < lanes:
        for k in range(4):
            at = slice(k * lanes + chi, (k + 1) * lanes)
            ms[:, :, :, at] = jnp.zeros((plan.pairs, plan.pairs, chi, lanes - chi), bf16)
    upper = [upper_rows[i : i + 1, :] for i in range(n)]
    for src, which in halves(mine, other):
        at = pl.multiple_of(which * half, 16)
        gap = bond_next - bond_col[pl.ds(at, half), :]
        for u in range(n):
            for v in range(n):
                keep = gap == upper[u] - upper[v]
                val = jnp.where(keep, src[u * n + v].astype(jnp.float32), 0.0)
                lane = (v % 2 * 2 + u % 2) * lanes
                ms[u // 2, v // 2, pl.ds(at, half), lane : lane + chi] = val.astype(bf16)
    pad = n * plan.lm
    w1[:, :, pad:, :] = jnp.zeros((2, plan.pairs, plan.cols2 - pad, w1.shape[3]), bf16)
    phases = [(o, vp, h) for o in range(3) for vp in range(plan.pairs) for h in range(2)]
    per_g = plan.groups // (2 * plan.pairs)
    chain, done = (w2_a, w2_b, w2), (w3_a, w3_b)

    def lead(o, vp, h):
        first(plan, quad_rows(lhs, plan, 2 * o + h), ms, w1.at[h], vp)

    lead(*phases[0])
    for i, (o, vp, h) in enumerate(phases):
        if i + 1 < len(phases):
            lead(*phases[i + 1])
        if o:
            at = (2 * vp + h) * per_g
            for g in range(at, at + per_g):
                third(plan, k3, chain[o - 1], done[o - 1], g)
        second(plan, k2, w1.at[h], chain[o], vp, h)


def middle_kernel(plan, lhs, ms, k2, k3, w2_in, w2, w3, w1):
    pad = plan.legs * plan.lm
    w1[:, :, pad:, :] = jnp.zeros((2, plan.pairs, plan.cols2 - pad, w1.shape[3]), jnp.bfloat16)
    phases = [(vp, h) for vp in range(plan.pairs) for h in range(2)]
    per_g = plan.groups // len(phases)

    def lead(vp, h):
        first(plan, quad_rows(lhs, plan, 6 + h), ms, w1.at[h], vp)

    lead(*phases[0])
    for i, (vp, h) in enumerate(phases):
        if i + 1 < len(phases):
            lead(*phases[i + 1])
        for g in range(i * per_g, (i + 1) * per_g):
            third(plan, k3, w2_in, w3, g)
        second(plan, k2, w1.at[h], w2, vp, h)


def back_kernel(
    plan,
    charges_s,
    charges_v, lhs, ms, k2, k3, w2_in, w3_a, w3_b, w3_c, pr_mine, pr_other,
    image, partial,
    pr, w1, w2_a, w2_b, w3_d, w3_e, w3_f,
):
    n, chi, half, lanes = plan.legs, plan.chi, plan.half, plan.lanes
    bf16 = jnp.bfloat16
    link_next = [charges_s[2, i] for i in range(n)]
    bond_next = charges_v[0:1, :]
    fresh_col = column_of(charges_v[1:2, :])
    pr[...] = jnp.zeros_like(pr)
    for src, which in halves(pr_mine, pr_other):
        at = pl.multiple_of(which * half, 16)
        gap = jnp.where(which == 0, fresh_col[:half], fresh_col[half:]) - bond_next
        for r in range(n):
            for s in range(n):
                keep = gap == link_next[r] - link_next[s]
                val = jnp.where(keep, src[r * n + s].astype(jnp.float32), 0.0)
                pr[r, pl.ds(at, half), s * lanes : s * lanes + chi] = val.astype(bf16)
    pad = n * plan.lm
    w1[:, :, pad:, :] = jnp.zeros((2, plan.pairs, plan.cols2 - pad, w1.shape[3]), bf16)

    block = 2 * QUAD * plan.xrows
    per_g = plan.groups // (2 * plan.pairs)
    per_r = n // (2 * plan.pairs)

    def put(oct, total):
        pieces = []
        for h in range(2):
            for x in range(QUAD):
                for dp in range(plan.pairs):
                    at = ((h * plan.pairs + dp) * QUAD + x) * plan.seg
                    pieces.append(total[at : at + plan.seg])
        image[oct * block : (oct + 1) * block, :] = jnp.concatenate(pieces, axis=0)
        return jnp.sum(total * total)

    w2 = (w2_in, w2_a, w2_b)
    w3 = (w3_a, w3_b, w3_c, w3_d, w3_e, w3_f)
    phases = [(o, vp, h) for o in range(2) for vp in range(plan.pairs) for h in range(2)]

    def lead(o, vp, h):
        first(plan, quad_rows(lhs, plan, 2 * (o + 4) + h), ms, w1.at[h], vp)

    square_sum = 0.0
    total = None
    lead(*phases[0])
    for i, (o, vp, h) in enumerate(phases):
        if i + 1 < len(phases):
            lead(*phases[i + 1])
        phase = 2 * vp + h
        for g in range(phase * per_g, (phase + 1) * per_g):
            third(plan, k3, w2[o], w3[o + 3], g)
        for r in range(phase * per_r, (phase + 1) * per_r):
            total = add(total, fourth(w3[o], pr, r))
        second(plan, k2, w1.at[h], w2[o + 1], vp, h)
        if phase == 2 * plan.pairs - 1:
            square_sum = square_sum + put(o, total)
            total = None
    partial[...] = jnp.full_like(partial, square_sum)

    @pl.when(lax.axis_index("sec") >= 0)
    def _():
        square_sum = 0.0
        total = None
        for g in range(plan.groups):
            third(plan, k3, w2[2], w3[5], g)
            if g % plan.pairs == 0:
                total = add(total, fourth(w3[2], pr, g // plan.pairs))
        square_sum = square_sum + put(2, total)
        for o in range(3, 6):
            even = odd = None
            for r in range(0, n, 2):
                even = add(even, fourth(w3[o], pr, r))
                odd = add(odd, fourth(w3[o], pr, r + 1))
            square_sum = square_sum + put(o, even + odd)
        partial[...] += jnp.full_like(partial, square_sum)


def finish_kernel(plan, count, columns, incoming, image, new, log_norm):
    n, half = plan.legs, plan.half
    sums = incoming[...]
    devices = sums.shape[0]
    row = lax.broadcasted_iota(jnp.int32, sums.shape, 0)
    pair = sums + pltpu.roll(sums, devices - 1, 0)
    logs = 0.5 * jnp.log(pair / count + 1e-06)
    log_norm[0, 0] = jnp.sum(jnp.where(row % 2 == 0, logs, 0.0)[:, :1]) / columns
    here = jnp.sum(jnp.where(row == 2 * lax.axis_index("col"), pair, 0.0), axis=0, keepdims=True)
    scale = lax.rsqrt(here / count + 1e-06)[:, : plan.chi]
    for d in range(n):
        for e in range(n):
            at = (d // 2) * plan.seg + (d % 2) * n + e
            new[d * n + e] = (image[pl.ds(at, half, stride=plan.xrows), :] * scale).astype(jnp.bfloat16)


def whole(memory, count):
    return [pl.BlockSpec(memory_space=memory) for _ in range(count)]


def absorb_row(mps, ket, left_proj, right_proj, bond_charge, new_charge, link_charge, vert_charge):
    half, chi, legs = left_proj.shape[1], left_proj.shape[2], left_proj.shape[3]
    phys = ket.shape[5]
    plan = Plan(chi, half, legs, phys)
    squared = legs * legs
    columns, sections = lax.axis_size("col"), lax.axis_size("sec")
    bf16, f32 = jnp.bfloat16, jnp.float32
    smem, vmem = pltpu.SMEM, pltpu.VMEM
    swap = [(i, 1 - i) for i in range(sections)]
    hbm = pltpu.HBM
    link_row = jnp.pad(link_charge, ((0, 0), (0, chi - legs)))
    charges = from_behind(jnp.concatenate([bond_charge, new_charge, link_row], axis=0), "col", -1)
    mine = jnp.transpose(mps[0], (1, 2, 0, 3)).reshape(squared, half, chi)
    other = lax.ppermute(mine, "sec", swap)
    pr_mine = from_behind(jnp.transpose(right_proj[0], (1, 2, 3, 0)).reshape(squared, half, chi), "col", -1)
    left = jnp.transpose(left_proj[0], (2, 3, 0, 1)).reshape(squared, half, chi)
    flat_ket = jnp.transpose(ket[0], (0, 1, 2, 4, 3)).reshape(squared, squared * phys)
    fetched = [left, bond_charge, new_charge, link_charge, vert_charge] + plan.matrices() + plan.indices() + [mine]
    in_smem = (3, 4)
    scratch = [(smem if i in in_smem else vmem)(x.shape, x.dtype) for i, x in enumerate(fetched[:-1])]
    lhs, *kets = pl.pallas_call(
        functools.partial(prep_kernel, plan),
        in_specs=whole(vmem, 1) + whole(hbm, len(fetched)),
        out_specs=whole(vmem, 8),
        out_shape=[
            jax.ShapeDtypeStruct((half * plan.lm, chi), bf16),
            jax.ShapeDtypeStruct((plan.rows2, plan.cols2), bf16),
            jax.ShapeDtypeStruct((plan.rows3, plan.cols3), bf16),
            jax.ShapeDtypeStruct((squared * phys, plan.cols2), jnp.int32),
            jax.ShapeDtypeStruct((plan.rows3, plan.cols3), jnp.int32),
            jax.ShapeDtypeStruct((chi, 1), jnp.int32),
            jax.ShapeDtypeStruct((round_up(legs, 8), chi), jnp.int32),
            jax.ShapeDtypeStruct(mine.shape, bf16),
        ],
        scratch_shapes=[pltpu.VMEM((half * plan.lm, chi), f32)] + scratch + [pltpu.SemaphoreType.DMA((len(fetched),))],
        compiler_params=pltpu.CompilerParams(vmem_limit_bytes=12 << 20),
        cost_estimate=pl.CostEstimate(flops=FRONT_FLOPS // 8, bytes_accessed=1 << 20, transcendentals=0),
        name="prep",
    )(flat_ket, *[pltpu.with_memory_space_constraint(x, pltpu.HBM) for x in fetched])
    octs = half // (2 * QUAD)
    if half % (2 * QUAD) or octs != 6 or (QUAD * chi) % LANES or QUAD * plan.seg % 16:
        raise ValueError("half")
    block = 2 * QUAD * plan.xrows
    lanes = plan.lanes
    wide = 2 * QUAD * chi
    w1_shape = (2, plan.pairs, plan.cols2, wide)
    w2_shape = jax.ShapeDtypeStruct((plan.groups, plan.cols3, wide), bf16)
    w3_shape = jax.ShapeDtypeStruct((legs, block, legs * lanes), bf16)
    operands = [charges, charges, other, lhs] + kets
    ms, k2, k3, w2, *w3 = pl.pallas_call(
        functools.partial(front_kernel, plan),
        in_specs=whole(smem, 1) + whole(vmem, len(operands) - 1),
        out_specs=whole(vmem, 6),
        out_shape=[
            jax.ShapeDtypeStruct((plan.pairs, plan.pairs, chi, 4 * lanes), bf16),
            jax.ShapeDtypeStruct((plan.rows2, plan.cols2), bf16),
            jax.ShapeDtypeStruct((plan.rows3, plan.cols3), bf16),
            w2_shape,
            w3_shape,
            w3_shape,
        ],
        scratch_shapes=[
            pltpu.VMEM(w1_shape, bf16),
            pltpu.VMEM(w2_shape.shape, bf16),
            pltpu.VMEM(w2_shape.shape, bf16),
        ],
        compiler_params=pltpu.CompilerParams(vmem_limit_bytes=VMEM_LIMIT),
        cost_estimate=pl.CostEstimate(flops=FRONT_FLOPS, bytes_accessed=1 << 20, transcendentals=0),
        name="front",
    )(*operands)
    pr_mine, w2 = lax.optimization_barrier((pr_mine, w2))
    pr_other = lax.ppermute(pr_mine, "sec", swap)
    w2, w3_last = pl.pallas_call(
        functools.partial(middle_kernel, plan),
        in_specs=whole(vmem, 5),
        out_specs=whole(vmem, 2),
        out_shape=[w2_shape, w3_shape],
        scratch_shapes=[pltpu.VMEM(w1_shape, bf16)],
        compiler_params=pltpu.CompilerParams(vmem_limit_bytes=20 << 20),
        cost_estimate=pl.CostEstimate(flops=FRONT_FLOPS, bytes_accessed=1 << 20, transcendentals=0),
        name="middle",
    )(lhs, ms, k2, k3, w2)
    operands = [charges, charges, lhs, ms, k2, k3, w2, *w3, w3_last, pr_mine, pr_other]
    image, partial = pl.pallas_call(
        functools.partial(back_kernel, plan),
        in_specs=whole(smem, 1) + whole(vmem, len(operands) - 1),
        out_specs=whole(vmem, 2),
        out_shape=[
            jax.ShapeDtypeStruct((octs * block, chi), f32),
            jax.ShapeDtypeStruct((columns * sections, 1, LANES), f32),
        ],
        scratch_shapes=[
            pltpu.VMEM((legs, chi, legs * lanes), bf16),
            pltpu.VMEM(w1_shape, bf16),
        ]
        + [pltpu.VMEM(w2_shape.shape, bf16)] * 2
        + [pltpu.VMEM(w3_shape.shape, bf16)] * 3,
        compiler_params=pltpu.CompilerParams(vmem_limit_bytes=VMEM_LIMIT),
        cost_estimate=pl.CostEstimate(flops=2 * FRONT_FLOPS, bytes_accessed=1 << 20, transcendentals=0),
        name="back",
    )(*operands)
    incoming = lax.all_to_all(partial, ("col", "sec"), 0, 0, tiled=True)
    new, log_norm = pl.pallas_call(
        functools.partial(finish_kernel, plan, float(chi * squared * chi), float(columns)),
        in_specs=whole(vmem, 2),
        out_specs=whole(vmem, 1) + whole(smem, 1),
        out_shape=[
            jax.ShapeDtypeStruct((squared, half, chi), bf16),
            jax.ShapeDtypeStruct((1, 1), f32),
        ],
        compiler_params=pltpu.CompilerParams(vmem_limit_bytes=8 << 20),
        name="finish",
    )(incoming.reshape(columns * sections, LANES), image)
    new_mps = jnp.transpose(new.reshape(legs, legs, half, chi), (2, 0, 1, 3))[None]
    return (new_mps, log_norm.reshape(()))


def solution(mesh):
    placed = (
        P("col", "sec", None, None, None),
        P("col", None, None, None, None, None),
        P("col", "sec", None, None, None),
        P("col", None, None, None, "sec"),
        P("col", None),
        P("col", None),
        P("col", None),
        P("col", None, None),
    )
    return jax.shard_map(
        absorb_row,
        mesh=mesh,
        in_specs=placed,
        out_specs=(P("col", "sec", None, None, None), P()),
        check_vma=False,
    )
```
